8 devices in a mesh: dp: 1 (over z), tp: 2 (over y), ep: 4 (over x, core).
Axes of the slice: x: 2, y: 2, z: 1, core: 2. Of those that a mesh axis runs over, the one named last changes fastest.
Arguments:
- tokens_a: bfloat16 [16384, 2048], P(('dp', 'ep', 'tp'))
- expert_ids_a: int32 [16384, 2], P(('dp', 'ep', 'tp'))
- gates_a: float32 [16384, 2], P(('dp', 'ep', 'tp'))
- tokens_b: bfloat16 [16384, 2048], P(('dp', 'ep', 'tp'))
- expert_ids_b: int32 [16384, 2], P(('dp', 'ep', 'tp'))
- gates_b: float32 [16384, 2], P(('dp', 'ep', 'tp'))
- w_gate: bfloat16 [8, 2048, 5632], P('ep', None, 'tp')
- w_up: bfloat16 [8, 2048, 5632], P('ep', None, 'tp')
- w_down: bfloat16 [8, 5632, 2048], P('ep', 'tp')
Outputs:
- output 1: bfloat16 [16384, 2048], P(('dp', 'ep', 'tp'))
- output 2: bfloat16 [16384, 2048], P(('dp', 'ep', 'tp'))
All inputs are finite; a program needn't handle non-finite values.
Results may differ from the reference program's by a relative error of at most 0.00149.
Values are sent between devices in bfloat16 or wider.
A program may use at most 1 GiB of HBM per device.

```python
import jax
import jax.numpy as jnp
from jax import lax

D_MODEL = 2048
D_FF = 5632
EXPERTS = 8
TOP_K = 2
TOK_DEV = 2048
SHARDS = 8

MEAN_LOAD = TOP_K * TOK_DEV // EXPERTS
CAPACITY = MEAN_LOAD + MEAN_LOAD // 4
TOKENS = SHARDS * TOK_DEV
STRIDE = EXPERTS // TOP_K
COPIES = TOK_DEV * TOP_K


def draw_routing(route_key):
    key_perm, key_rand, key_coin = jax.random.split(route_key, 3)
    perm_keys = jax.random.split(key_perm, SHARDS)
    perm_ranks = jax.vmap(lambda one_key: jax.random.permutation(one_key, TOK_DEV))(perm_keys)
    wild_ids = jax.random.randint(key_rand, (SHARDS, TOK_DEV), 0, EXPERTS)
    coin_flip = jax.random.randint(key_coin, (SHARDS, TOK_DEV), 0, 2)
    take_even = (coin_flip == 1) | (perm_ranks < EXPERTS)
    base_ids = jnp.where(take_even, perm_ranks % EXPERTS, wild_ids).reshape(TOKENS)
    offsets = jnp.arange(TOP_K) * STRIDE
    return ((base_ids[:, None] + offsets[None, :]) % EXPERTS).astype(jnp.int32)


def setup_inputs(seed: int = 0, part: int = 0) -> dict:
    part_keys = jax.random.split(jax.random.fold_in(jax.random.key(seed), part), 6)
    weight_keys = jax.random.split(jax.random.key(seed + 1), 3)

    def draw_batch(tok_key, route_key, gate_key):
        tokens = jax.random.normal(tok_key, (TOKENS, D_MODEL), jnp.float32).astype(jnp.bfloat16)
        gate_vals = jax.random.uniform(gate_key, (TOKENS, TOP_K), jnp.float32, 0.25, 1.75) * TOP_K ** -0.5
        return tokens, draw_routing(route_key), gate_vals

    tokens_a, expert_ids_a, gates_a = draw_batch(part_keys[0], part_keys[1], part_keys[2])
    tokens_b, expert_ids_b, gates_b = draw_batch(part_keys[3], part_keys[4], part_keys[5])
    w_gate = (jax.random.normal(weight_keys[0], (EXPERTS, D_MODEL, D_FF), jnp.float32) * D_MODEL ** -0.5).astype(jnp.bfloat16)
    w_up = (jax.random.normal(weight_keys[1], (EXPERTS, D_MODEL, D_FF), jnp.float32) * D_MODEL ** -0.5).astype(jnp.bfloat16)
    w_down = (jax.random.normal(weight_keys[2], (EXPERTS, D_FF, D_MODEL), jnp.float32) * D_FF ** -0.5).astype(jnp.bfloat16)
    return {"tokens_a": tokens_a, "expert_ids_a": expert_ids_a, "gates_a": gates_a, "tokens_b": tokens_b, "expert_ids_b": expert_ids_b, "gates_b": gates_b, "w_gate": w_gate, "w_up": w_up, "w_down": w_down}


def slot_index(flat_ids):
    onehot = (flat_ids[:, None] == jnp.arange(EXPERTS)[None, :]).astype(jnp.int32)
    position = jnp.sum(jnp.cumsum(onehot, axis=0) * onehot, axis=1) - 1
    return jnp.where(position < CAPACITY, flat_ids * CAPACITY + position, EXPERTS * CAPACITY)


def fill_slots(block_rows, slot_ids):
    copy_tok = (jnp.arange(COPIES) // TOP_K).astype(jnp.int32)
    source = jnp.full((EXPERTS * CAPACITY,), TOK_DEV, jnp.int32).at[slot_ids].set(copy_tok, mode="drop")
    return jnp.take(block_rows, source, axis=0, mode="fill", fill_value=0)


def pick_rows(out_rows, slot_ids):
    return jnp.take(out_rows, slot_ids, axis=0, mode="fill", fill_value=0)


def expert_ffn(operands):
    rows_in, gate_w, up_w, down_w = operands
    gate_act = jnp.dot(rows_in, gate_w, preferred_element_type=jnp.float32)
    up_lin = jnp.dot(rows_in, up_w, preferred_element_type=jnp.float32)
    hidden = (jax.nn.silu(gate_act) * up_lin).astype(jnp.bfloat16)
    return jnp.dot(hidden, down_w, preferred_element_type=jnp.float32).astype(jnp.bfloat16)


def moe_layer(tokens, expert_ids, gate_vals, w_gate, w_up, w_down):
    blocks = tokens.reshape(SHARDS, TOK_DEV, D_MODEL)
    flat_ids = expert_ids.reshape(SHARDS, COPIES)
    slot_ids = jax.vmap(slot_index)(flat_ids)
    slot_rows = jax.vmap(fill_slots)(blocks, slot_ids)
    per_expert = slot_rows.reshape(SHARDS, EXPERTS, CAPACITY, D_MODEL).transpose(1, 0, 2, 3).reshape(EXPERTS, SHARDS * CAPACITY, D_MODEL)
    results = lax.map(expert_ffn, (per_expert, w_gate, w_up, w_down))
    back_rows = results.reshape(EXPERTS, SHARDS, CAPACITY, D_MODEL).transpose(1, 0, 2, 3).reshape(SHARDS, EXPERTS * CAPACITY, D_MODEL)
    copies = jax.vmap(pick_rows)(back_rows, slot_ids)
    weighted = copies.reshape(SHARDS, TOK_DEV, TOP_K, D_MODEL).astype(jnp.float32) * gate_vals.reshape(SHARDS, TOK_DEV, TOP_K, 1)
    return jnp.sum(weighted, axis=2).reshape(TOKENS, D_MODEL).astype(jnp.bfloat16)


def reference(tokens_a, expert_ids_a, gates_a, tokens_b, expert_ids_b, gates_b, w_gate, w_up, w_down):
    out_a = moe_layer(tokens_a, expert_ids_a, gates_a, w_gate, w_up, w_down)
    out_b = moe_layer(tokens_b, expert_ids_b, gates_b, w_gate, w_up, w_down)
    return (out_a, out_b)
```

```python
import jax
import jax.numpy as jnp
from jax import lax
from jax.sharding import PartitionSpec as P


TP_SWAP = [(0, 1), (1, 0)]
BF16 = jnp.bfloat16
F32 = jnp.float32


def solution(mesh):
    ep_size = mesh.shape["ep"]
    row_spec = P(("dp", "ep", "tp"), None)
    gate_spec = P("ep", None, "tp")
    down_spec = P("ep", "tp", None)

    def ep_swap(value, mask):
        return lax.ppermute(value, "ep", [(i, i ^ mask) for i in range(ep_size)])

    def tp_swap(value):
        return lax.ppermute(value, "tp", TP_SWAP)

    def mm(a, b):
        return jnp.einsum("krd,kdf->krf", a, b, preferred_element_type=F32)

    def routing(expert_ids, me):
        tok_loc, top_k = expert_ids.shape
        num_experts = 2 * ep_size
        mean_load = top_k * tok_loc // num_experts
        capacity = mean_load + mean_load // 4
        flat_ids = expert_ids.reshape(tok_loc * top_k)
        onehot = (flat_ids[:, None] == jnp.arange(num_experts, dtype=jnp.int32)[None, :]).astype(jnp.int32)
        position = jnp.sum(jnp.cumsum(onehot, axis=0) * onehot, axis=1) - 1
        kept = position < capacity
        slot = (((flat_ids // 2) ^ me) * 2 + flat_ids % 2) * capacity + position
        slot = jnp.where(kept, slot, num_experts * capacity)
        copy_tok = jnp.arange(tok_loc * top_k, dtype=jnp.int32) // top_k
        source = jnp.full((num_experts * capacity,), tok_loc, jnp.int32).at[slot].set(copy_tok, mode="drop")
        return source.reshape(ep_size, 2 * capacity), slot

    def group_body(tokens_a, ids_a, gates_a, tokens_b, ids_b, gates_b, w_gate, w_up, w_down):
        me = lax.axis_index("ep")
        model = w_down.shape[2]
        g_r, u_r, d_r = tp_swap(w_gate), tp_swap(w_up), tp_swap(w_down)

        def dispatch(tokens, ids):
            source, slot = routing(ids, me)
            rows = [jnp.take(tokens, source[m], axis=0, mode="fill", fill_value=0) for m in range(ep_size)]
            rows = [r if m == 0 else ep_swap(r, m) for m, r in enumerate(rows)]
            return jnp.concatenate([r.reshape(2, -1, model) for r in rows], axis=1), slot

        def hidden(x, wg, wu):
            return (jax.nn.silu(mm(x, wg)) * mm(x, wu)).astype(BF16)

        def finish(y, slot, gates):
            parts = jnp.split(y, ep_size, axis=1)
            ret = jnp.concatenate([p if m == 0 else ep_swap(p, m) for m, p in enumerate(parts)], axis=0)
            copies = jnp.take(ret.reshape(-1, model), slot, axis=0, mode="fill", fill_value=0)
            weighted = copies.reshape(gates.shape + (model,)).astype(F32) * gates[:, :, None]
            return jnp.sum(weighted, axis=1).astype(BF16)

        x_a, slot_a = dispatch(tokens_a, ids_a)
        x_b, slot_b = dispatch(tokens_b, ids_b)
        h_a, h_b = hidden(x_a, w_gate, w_up), hidden(x_b, w_gate, w_up)
        p_a, p_b = mm(h_a, w_down), mm(h_b, w_down)
        h_a, h_b = hidden(x_a, g_r, u_r), hidden(x_b, g_r, u_r)
        y_a = (p_a + mm(h_a, d_r)).astype(BF16)
        y_b = (p_b + mm(h_b, d_r)).astype(BF16)
        return finish(y_a, slot_a, gates_a), finish(y_b, slot_b, gates_b)

    in_specs = (row_spec, row_spec, row_spec, row_spec, row_spec, row_spec, gate_spec, gate_spec, down_spec)
    return jax.shard_map(group_body, mesh=mesh, in_specs=in_specs, out_specs=(row_spec, row_spec), check_vma=False)
```

```python
import functools

import jax
import jax.numpy as jnp
from jax import lax
from jax.experimental import pallas as pl
from jax.experimental.pallas import tpu as pltpu
from jax.sharding import PartitionSpec as P


TP_SWAP = [(0, 1), (1, 0)]
BF16 = jnp.bfloat16
F32 = jnp.float32
MASKS = 4
TN = 256
VMEM_LIMIT = 60 * 1024 * 1024


def mm(a, b):
    return jnp.dot(a, b, preferred_element_type=F32)


def call(kernel, flops, nbytes, **kw):
    params = pltpu.CompilerParams(vmem_limit_bytes=VMEM_LIMIT)
    cost = pl.CostEstimate(flops=int(flops), bytes_accessed=int(nbytes), transcendentals=0)
    return pl.pallas_call(kernel, compiler_params=params, cost_estimate=cost, **kw)


def any_spec():
    return pl.BlockSpec(memory_space=pl.ANY)


def dispatch_kernel(pos_ref, tok_ref, *outs):
    step = pl.program_id(0)
    cap, model = outs[0].shape[1:]
    slots = lax.broadcasted_iota(jnp.int32, (cap, tok_ref.shape[0]), 0)
    onehot = (slots == pos_ref[0]).astype(BF16)
    for m, out in enumerate(outs):

        @pl.when(step // 2 == m)
        def _():
            for lo in range(0, model, 512):
                out[0, :, lo:lo + 512] = mm(onehot, tok_ref[:, lo:lo + 512]).astype(BF16)


def dispatch(pos, tokens, cap):
    n = pos.shape[0] // 2
    toks, model = tokens.shape
    out = jax.ShapeDtypeStruct((2, cap, model), BF16)
    return call(
        dispatch_kernel, 2 * n * 2 * cap * toks * model, toks * model * 2 + 2 * n * cap * model * 2,
        grid=(2 * n,),
        in_specs=[pl.BlockSpec((1, 1, toks), lambda i: (i, 0, 0)), pl.BlockSpec((toks, model), lambda i: (0, 0))],
        out_specs=[pl.BlockSpec((1, cap, model), functools.partial(lambda m, i: (jnp.clip(i - 2 * m, 0, 1), 0, 0), m)) for m in range(n)],
        out_shape=[out] * n,
    )(pos, tokens)


def hidden_kernel(*refs):
    xs, (wg, wu), h = refs[:MASKS], refs[MASKS:MASKS + 2], refs[-1]
    g = wg[...].reshape(wg.shape[-2:])
    u = wu[...].reshape(wu.shape[-2:])
    for m in range(MASKS):
        x = xs[m][0]
        a = mm(x, g)
        h[m] = (a * jax.nn.sigmoid(a) * mm(x, u)).astype(BF16)


def weight_spec(w, k, cols, off):
    if w.ndim == 3:
        return pl.BlockSpec((1, w.shape[1], cols), lambda n: (k, 0, n + off))
    return pl.BlockSpec((w.shape[0], cols), lambda n: (0, n + off))


def hidden(xs, wg, wu, k, width, off=0, wu_off=0, steps=None, into=None):
    _, cap, model = xs[0].shape
    steps = width // TN if steps is None else steps
    in_specs = [pl.BlockSpec((1, cap, model), lambda n: (k, 0, 0)) for _ in xs]
    in_specs += [weight_spec(wg, k, TN, off), weight_spec(wu, k, TN, wu_off)]
    args = [*xs, wg, wu]
    kw = {}
    if into is not None:
        args.append(into)
        in_specs.append(any_spec())
        kw["input_output_aliases"] = {len(args) - 1: 0}
    rows = MASKS * cap
    return call(
        hidden_kernel, 4 * rows * model * TN * steps, 2 * (rows * model + 2 * model * TN * steps + rows * TN * steps),
        grid=(steps,), in_specs=in_specs,
        out_specs=pl.BlockSpec((MASKS, cap, TN), lambda n: (0, 0, n + off)),
        out_shape=jax.ShapeDtypeStruct((MASKS, cap, width), BF16), **kw,
    )(*args)


def part_kernel(h, wd, out):
    for m in range(MASKS):
        out[m] = mm(h[m], wd[0])


def part(h, wd, k):
    _, cap, width = h.shape
    model = wd.shape[2]
    rows = MASKS * cap
    return call(
        part_kernel, 2 * rows * width * model, 2 * (rows * width + width * model) + 4 * rows * model,
        grid=(model // TN,),
        in_specs=[pl.BlockSpec((MASKS, cap, width), lambda n: (0, 0, 0)), pl.BlockSpec((1, width, TN), lambda n: (k, 0, n))],
        out_specs=pl.BlockSpec((MASKS, cap, TN), lambda n: (0, 0, n)),
        out_shape=jax.ShapeDtypeStruct((MASKS, cap, model), F32),
    )(h, wd)


def final_kernel(h_a, h_b, p_a, p_b, wd, *outs):
    i = pl.program_id(0)
    for b, (h, p) in enumerate(((h_a, p_a), (h_b, p_b))):
        for m, out in enumerate(outs):

            @pl.when(i == b * MASKS + m)
            def _():
                out[0] = (p[0] + mm(h[0], wd[...])).astype(BF16)


def final(h_a, h_b, p_a, p_b, wd, lo):
    _, cap, width = h_a.shape
    cols = wd.shape[1]
    first = lambda i: jnp.minimum(i, MASKS - 1)
    second = lambda i: jnp.maximum(i - MASKS, 0)
    at = lo // cols
    rows = 2 * MASKS * cap
    return call(
        final_kernel, 2 * rows * width * cols, 2 * (rows * width + width * cols) + 6 * rows * cols,
        grid=(2 * MASKS,),
        in_specs=[
            pl.BlockSpec((1, cap, width), lambda i: (first(i), 0, 0)),
            pl.BlockSpec((1, cap, width), lambda i: (second(i), 0, 0)),
            pl.BlockSpec((1, cap, cols), lambda i: (first(i), 0, at)),
            pl.BlockSpec((1, cap, cols), lambda i: (second(i), 0, at)),
            pl.BlockSpec((width, cols), lambda i: (0, 0)),
        ],
        out_specs=[pl.BlockSpec((1, cap, cols), functools.partial(lambda m, i: (jnp.where(i >= MASKS + m, 1, 0), 0, 0), m)) for m in range(MASKS)],
        out_shape=[jax.ShapeDtypeStruct((2, cap, cols), BF16)] * MASKS,
    )(h_a, h_b, p_a, p_b, wd)


TB = 512


def picked(k, ys, pos, gate):
    slots = lax.broadcasted_iota(jnp.int32, (TB, ys[0].shape[1]), 1)
    total = None
    for m in range(MASKS):
        e = 2 * m + k
        onehot = (slots == pos[0, :, e:e + 1]).astype(BF16)
        term = gate[0, :, e:e + 1] * mm(onehot, ys[m][0])
        total = term if total is None else total + term
    return total


def combine_first_kernel(k, *refs):
    refs[-1][...] = picked(k, refs[:MASKS], refs[MASKS], refs[MASKS + 1])


def combine_kernel(k, *refs):
    acc, outs = refs[MASKS + 2], refs[-2:]
    i, blocks = pl.program_id(0), pl.num_programs(0) // 2
    total = acc[...] + picked(k, refs[:MASKS], refs[MASKS], refs[MASKS + 1])
    for b, out in enumerate(outs):

        @pl.when(i // blocks == b)
        def _():
            out[...] = total.astype(BF16)


def combine(ys, pos, gate, k, lo, acc, into):
    _, cap, cols = ys[0].shape
    toks = pos.shape[1]
    blocks = toks // TB
    model = acc.shape[1]
    at = lo // cols
    in_specs = [pl.BlockSpec((1, cap, cols), lambda i: (i // blocks, 0, 0)) for _ in ys]
    in_specs += [pl.BlockSpec((1, TB, pos.shape[2]), lambda i: (i // blocks, i % blocks, 0))] * 2
    args = [*ys, pos, gate]
    args.append(acc)
    in_specs.append(pl.BlockSpec((TB, cols), lambda i: (i, at)))
    out_specs = [
        pl.BlockSpec((TB, cols), lambda i: (jnp.minimum(i, blocks - 1), at)),
        pl.BlockSpec((TB, cols), lambda i: (jnp.maximum(i - blocks, 0), at)),
    ]
    kw = {}
    if into is not None:
        for j, buf in enumerate(into):
            args.append(buf)
            in_specs.append(any_spec())
            kw.setdefault("input_output_aliases", {})[len(args) - 1] = j
    return call(
        functools.partial(combine_kernel, k), 2 * 2 * toks * MASKS * cap * cols, 2 * toks * cols * 6,
        grid=(2 * blocks,), in_specs=in_specs, out_specs=out_specs,
        out_shape=[jax.ShapeDtypeStruct((toks, model), BF16)] * 2, **kw,
    )(*args)


def combine_first(ys, pos, gate, k, lo, model, into):
    _, cap, cols = ys[0].shape
    toks = pos.shape[1]
    blocks = toks // TB
    at = lo // cols
    in_specs = [pl.BlockSpec((1, cap, cols), lambda i: (i // blocks, 0, 0)) for _ in ys]
    in_specs += [pl.BlockSpec((1, TB, pos.shape[2]), lambda i: (i // blocks, i % blocks, 0))] * 2
    args = [*ys, pos, gate]
    kw = {}
    if into is not None:
        args.append(into)
        in_specs.append(any_spec())
        kw["input_output_aliases"] = {len(args) - 1: 0}

    return call(
        functools.partial(combine_first_kernel, k), 2 * 2 * toks * MASKS * cap * cols, 2 * toks * cols * 6,
        grid=(2 * blocks,), in_specs=in_specs,
        out_specs=pl.BlockSpec((TB, cols), lambda i: (i, at)),
        out_shape=jax.ShapeDtypeStruct((2 * toks, model), F32), **kw,
    )(*args)


def cuts(sizes):
    out, at = [], 0
    for size in sizes:
        out.append((at, at + size))
        at += size
    return out


def solution(mesh):
    ep_size = mesh.shape["ep"]
    row_spec = P(("dp", "ep", "tp"), None)
    gate_spec = P("ep", None, "tp")
    down_spec = P("ep", "tp", None)

    def ep_swap(value, mask):
        return lax.ppermute(value, "ep", [(i, i ^ mask) for i in range(ep_size)])

    def tp_swap(value):
        return lax.ppermute(value, "tp", TP_SWAP)

    def routing(ids, gates, me):
        toks, top_k = ids.shape[1:]
        n_exp = 2 * ep_size
        mean_load = top_k * toks // n_exp
        cap = mean_load + mean_load // 4
        code = ((ids // 2) ^ me) * 2 + ids % 2
        hit = code[:, None] == jnp.arange(n_exp, dtype=jnp.int32)[None, :, None, None]
        has = jnp.any(hit, axis=3)
        count = has.astype(jnp.int32)
        pos = jnp.cumsum(count, axis=2) - count
        pos = jnp.where(has & (pos < cap), pos, -1)
        gate = jnp.sum(jnp.where(hit, gates[:, None], 0.0), axis=3)
        return pos, gate, cap

    def group_body(tokens_a, ids_a, gates_a, tokens_b, ids_b, gates_b, w_gate, w_up, w_down):
        me = lax.axis_index("ep")
        width, model = w_down.shape[1:]
        up_cuts = cuts([1024, 1024, 512, 256])
        d0_cuts = cuts([1024, 1024])
        d1_cuts = cuts([128, 128] + [256] * 6 + [128, 128])
        g_r = tp_swap(w_gate)
        u0_r = tp_swap(w_up[0])
        d0_r = [tp_swap(w_down[0][:, lo:hi]) for lo, hi in d0_cuts]
        u1_r = [tp_swap(w_up[1][:, lo:hi]) for lo, hi in up_cuts]
        d1_r = [tp_swap(w_down[1][:, lo:hi]) for lo, hi in d1_cuts]

        pos, gate, cap = routing(jnp.stack([ids_a, ids_b]), jnp.stack([gates_a, gates_b]), me)
        pos_t, gate_t = pos.transpose(0, 2, 1), gate.transpose(0, 2, 1)

        xs = []
        for b, tokens in enumerate((tokens_a, tokens_b)):
            rows = pos[b][:, None, :]
            far = dispatch(rows[4:], tokens, cap)
            far = [ep_swap(far[0], 2), ep_swap(far[1], 3)]
            near = dispatch(rows[:4], tokens, cap)
            xs.append([near[0], ep_swap(near[1], 1), *far])

        def bring_back(ys):
            return [ys[0], ep_swap(ys[1], 1), ep_swap(ys[2], 2), ep_swap(ys[3], 3)]

        h_l, p = [[None] * 2, [None] * 2], [[None] * 2, [None] * 2]
        for b in range(2):
            for k in range(2):
                h_l[b][k] = hidden(xs[b], w_gate, w_up, k, width)
            for k in range(2):
                p[b][k] = part(h_l[b][k], w_down, k)

        h_r = []
        for b in range(2):
            h_r.append(hidden(xs[b], g_r, u0_r, 0, width))
        acc = None
        for n, (lo, hi) in enumerate(d0_cuts):
            ys = final(h_r[0], h_r[1], p[0][0], p[1][0], d0_r[n], lo)
            ys = bring_back(ys)
            acc = combine_first(ys, pos_t, gate_t, 0, lo, model, acc)

        h_r = [None, None]
        for n, (lo, hi) in enumerate(up_cuts):
            for b in range(2):
                h_r[b] = hidden(xs[b], g_r, u1_r[n], 1, width, lo // TN, steps=(hi - lo) // TN, into=h_r[b])
        outs = None
        for n, (lo, hi) in enumerate(d1_cuts):
            ys = final(h_r[0], h_r[1], p[0][1], p[1][1], d1_r[n], lo)
            ys = bring_back(ys)
            outs = combine(ys, pos_t, gate_t, 1, lo, acc, outs)
        return tuple(outs)

    in_specs = (row_spec, row_spec, row_spec, row_spec, row_spec, row_spec, gate_spec, gate_spec, down_spec)
    return jax.shard_map(group_body, mesh=mesh, in_specs=in_specs, out_specs=(row_spec, row_spec), check_vma=False)
```

```python
import functools

import jax
import jax.numpy as jnp
from jax import lax
from jax.experimental import pallas as pl
from jax.experimental.pallas import tpu as pltpu
from jax.sharding import PartitionSpec as P


TP_SWAP = [(0, 1), (1, 0)]
BF16 = jnp.bfloat16
F32 = jnp.float32
MASKS = 4
TN = 256
TB = 512
VMEM_LIMIT = 60 * 1024 * 1024


def mm(a, b):
    return jnp.dot(a, b, preferred_element_type=F32)


def call(kernel, flops, nbytes, **kw):
    params = pltpu.CompilerParams(vmem_limit_bytes=VMEM_LIMIT)
    cost = pl.CostEstimate(flops=int(flops), bytes_accessed=int(nbytes), transcendentals=0)
    return pl.pallas_call(kernel, compiler_params=params, cost_estimate=cost, **kw)


def filled_further(into, args, in_specs):
    if into is None:
        return {}
    args.append(into)
    in_specs.append(pl.BlockSpec(memory_space=pl.ANY))
    return {"input_output_aliases": {len(args) - 1: 0}}


def dispatch_kernel(pos_ref, tok_ref, *outs):
    step = pl.program_id(0)
    cap, model = outs[0].shape[1:]
    slots = lax.broadcasted_iota(jnp.int32, (cap, tok_ref.shape[0]), 0)
    onehot = (slots == pos_ref[0]).astype(BF16)
    for lo in range(0, model, 512):
        rows = mm(onehot, tok_ref[:, lo:lo + 512]).astype(BF16)
        for m, out in enumerate(outs):

            @pl.when(step // 2 == m)
            def _():
                out[0, :, lo:lo + 512] = rows


def dispatch(pos, tokens, cap):
    n = pos.shape[0] // 2
    toks, model = tokens.shape
    out = jax.ShapeDtypeStruct((2, cap, model), BF16)
    return call(
        dispatch_kernel, 2 * n * 2 * cap * toks * model, toks * model * 2 + 2 * n * cap * model * 2,
        grid=(2 * n,),
        in_specs=[pl.BlockSpec((1, 1, toks), lambda i: (i, 0, 0)), pl.BlockSpec((toks, model), lambda i: (0, 0))],
        out_specs=[pl.BlockSpec((1, cap, model), functools.partial(lambda m, i: (jnp.clip(i - 2 * m, 0, 1), 0, 0), m)) for m in range(n)],
        out_shape=[out] * n,
    )(pos, tokens)


def hidden_kernel(*refs):
    xs, (wg, wu), h = refs[:MASKS], refs[MASKS:MASKS + 2], refs[-1]
    g = wg[...].reshape(wg.shape[-2:])
    u = wu[...].reshape(wu.shape[-2:])
    for m in range(MASKS):
        x = xs[m][0]
        a = mm(x, g)
        h[0, m] = (a * jax.nn.sigmoid(a) * mm(x, u)).astype(BF16)


def hidden_local(xs, wg, wu):
    _, cap, model = xs[0].shape
    width = wg.shape[2]
    rows = 2 * MASKS * cap
    return call(
        hidden_kernel, 4 * rows * model * width, 2 * (rows * model + 4 * model * width + rows * width),
        grid=(2, width // TN),
        in_specs=[pl.BlockSpec((1, cap, model), lambda k, n: (k, 0, 0)) for _ in xs]
        + [pl.BlockSpec((1, model, TN), lambda k, n: (k, 0, n))] * 2,
        out_specs=pl.BlockSpec((1, MASKS, cap, TN), lambda k, n: (k, 0, 0, n)),
        out_shape=jax.ShapeDtypeStruct((2, MASKS, cap, width), BF16),
    )(*xs, wg, wu)


def hidden(xs, b, k, wg, wu, lo, into):
    _, cap, model = xs[0].shape
    width, cols = wg.shape[1], wu.shape[1]
    off, steps = lo // TN, cols // TN
    in_specs = [pl.BlockSpec((1, cap, model), lambda n: (k, 0, 0)) for _ in xs]
    in_specs += [pl.BlockSpec((model, TN), lambda n: (0, n + off)), pl.BlockSpec((model, TN), lambda n: (0, n))]
    args = [*xs, wg, wu]
    kw = filled_further(into, args, in_specs)
    rows = MASKS * cap
    return call(
        hidden_kernel, 4 * rows * model * cols, 2 * (rows * model + 2 * model * cols + rows * cols),
        grid=(steps,), in_specs=in_specs,
        out_specs=pl.BlockSpec((1, MASKS, cap, TN), lambda n: (b, 0, 0, n + off)),
        out_shape=jax.ShapeDtypeStruct((2, MASKS, cap, width), BF16), **kw,
    )(*args)


def part_kernel(h, wd, *refs):
    for m in range(MASKS):
        refs[-1][0, 0, m] = mm(h[0, m], wd[0])


def part(h, b, wd, into):
    _, _, cap, width = h.shape
    model = wd.shape[2]
    rows = 2 * MASKS * cap
    in_specs = [pl.BlockSpec((1, MASKS, cap, width), lambda k, n: (k, 0, 0, 0)), pl.BlockSpec((1, width, TN), lambda k, n: (k, 0, n))]
    args = [h, wd]
    kw = filled_further(into, args, in_specs)
    return call(
        part_kernel, 2 * rows * width * model, 2 * (rows * width + 2 * width * model) + 4 * rows * model,
        grid=(2, model // TN), in_specs=in_specs,
        out_specs=pl.BlockSpec((1, 1, MASKS, cap, TN), lambda k, n: (k, b, 0, 0, n)),
        out_shape=jax.ShapeDtypeStruct((2, 2, MASKS, cap, model), F32), **kw,
    )(*args)


def final_kernel(h, p, wd, *outs):
    m = pl.program_id(0) % len(outs)
    cap = h.shape[2]
    for lo in range(0, cap, cap // 2):
        rows = slice(lo, lo + cap // 2)
        y = (p[0, 0, 0, rows] + mm(h[0, 0, rows], wd[...])).astype(BF16)
        for j, out in enumerate(outs):

            @pl.when(m == j)
            def _():
                out[0, rows] = y


def final(h, p, k, wd, lo, masks):
    _, _, cap, width = h.shape
    cols = wd.shape[1]
    at, n, m0 = lo // cols, len(masks), masks[0]
    rows = 2 * n * cap
    return call(
        final_kernel, 2 * rows * width * cols, 2 * (rows * width + width * cols) + 6 * rows * cols,
        grid=(2 * n,),
        in_specs=[
            pl.BlockSpec((1, 1, cap, width), lambda i: (i // n, m0 + i % n, 0, 0)),
            pl.BlockSpec((1, 1, 1, cap, cols), lambda i: (k, i // n, m0 + i % n, 0, at)),
            pl.BlockSpec((width, cols), lambda i: (0, 0)),
        ],
        out_specs=[pl.BlockSpec((1, cap, cols), functools.partial(lambda m, i: (jnp.where(i >= n + m, 1, 0), 0, 0), m)) for m in range(n)],
        out_shape=[jax.ShapeDtypeStruct((2, cap, cols), BF16)] * n,
    )(h, p, wd)


def picked(k, ys, pick, gate):
    total = None
    for m in range(MASKS):
        e = 2 * m + k
        term = gate[0, :, e:e + 1] * mm(pick[0, m], ys[m][0])
        total = term if total is None else total + term
    return total


def combine_first_kernel(k, *refs):
    refs[-1][...] = picked(k, refs[:MASKS], refs[MASKS], refs[MASKS + 1])


def combine_kernel(k, *refs):
    acc, outs = refs[MASKS + 2], refs[-2:]
    i, blocks = pl.program_id(0), pl.num_programs(0) // 2
    total = (acc[...] + picked(k, refs[:MASKS], refs[MASKS], refs[MASKS + 1])).astype(BF16)
    for b, out in enumerate(outs):

        @pl.when(i // blocks == b)
        def _():
            out[...] = total


def combine(ys, pick, gate, k, lo, model, acc=None, into=None):
    _, cap, cols = ys[0].shape
    toks = pick.shape[2]
    blocks = toks // TB
    at = lo // cols
    in_specs = [pl.BlockSpec((1, cap, cols), lambda i: (i // blocks, 0, 0)) for _ in ys]
    in_specs += [
        pl.BlockSpec((1, MASKS, TB, cap), lambda i: (i // blocks, 0, i % blocks, 0)),
        pl.BlockSpec((1, TB, gate.shape[2]), lambda i: (i // blocks, i % blocks, 0)),
    ]
    args = [*ys, pick, gate]
    flops, nbytes = 2 * 2 * toks * MASKS * cap * cols, 2 * 2 * toks * MASKS * cap + 2 * toks * cols * 6
    if acc is None:
        kw = filled_further(into, args, in_specs)
        return call(
            functools.partial(combine_first_kernel, k), flops, nbytes,
            grid=(2 * blocks,), in_specs=in_specs,
            out_specs=pl.BlockSpec((TB, cols), lambda i: (i, at)),
            out_shape=jax.ShapeDtypeStruct((2 * toks, model), F32), **kw,
        )(*args)
    args.append(acc)
    in_specs.append(pl.BlockSpec((TB, cols), lambda i: (i, at)))
    kw = {}
    if into is not None:
        kw["input_output_aliases"] = {len(args): 0, len(args) + 1: 1}
        args += into
        in_specs += [pl.BlockSpec(memory_space=pl.ANY)] * 2
    return call(
        functools.partial(combine_kernel, k), flops, nbytes,
        grid=(2 * blocks,), in_specs=in_specs,
        out_specs=[
            pl.BlockSpec((TB, cols), lambda i: (jnp.minimum(i, blocks - 1), at)),
            pl.BlockSpec((TB, cols), lambda i: (jnp.maximum(i - blocks, 0), at)),
        ],
        out_shape=[jax.ShapeDtypeStruct((toks, model), BF16)] * 2, **kw,
    )(*args)


def cuts(sizes):
    out, at = [], 0
    for size in sizes:
        out.append((at, at + size))
        at += size
    return out


def solution(mesh):
    ep_size = mesh.shape["ep"]
    row_spec = P(("dp", "ep", "tp"), None)
    gate_spec = P("ep", None, "tp")
    down_spec = P("ep", "tp", None)
    up1_cuts = cuts([512, 1024, 1024, 256])
    down_cuts = [cuts([1024] + [256] * 4), cuts([256] * 7 + [128, 128])]
    late = [(0, n) for n in range(1, 5)] + [(1, n) for n in range(9)]
    halves = [(1, 7), (1, 8)]

    def ep_swap(value, mask):
        return lax.ppermute(value, "ep", [(i, i ^ mask) for i in range(ep_size)])

    def tp_swap(w, k, lo=0, hi=None):
        piece = lax.slice(w, (k, 0, lo), (k + 1, w.shape[1], w.shape[2] if hi is None else hi))
        return lax.ppermute(piece, "tp", TP_SWAP)[0]

    def routing(ids, gates, me):
        toks, top_k = ids.shape[1:]
        n_exp = 2 * ep_size
        mean_load = top_k * toks // n_exp
        cap = mean_load + mean_load // 4
        code = ((ids // 2) ^ me) * 2 + ids % 2
        hit = code[:, None] == jnp.arange(n_exp, dtype=jnp.int32)[None, :, None, None]
        has = jnp.any(hit, axis=3)
        count = has.astype(jnp.int32)
        pos = jnp.cumsum(count, axis=2) - count
        pos = jnp.where(has & (pos < cap), pos, -1)
        gate = jnp.sum(jnp.where(hit, gates[:, None], 0.0), axis=3)
        return pos, gate, cap

    def group_body(tokens_a, ids_a, gates_a, tokens_b, ids_b, gates_b, w_gate, w_up, w_down):
        me = lax.axis_index("ep")
        model = w_down.shape[2]
        up1 = [None] * len(up1_cuts)
        up1[0] = tp_swap(w_up, 1, *up1_cuts[0])
        gate0 = tp_swap(w_gate, 0)
        up0 = tp_swap(w_up, 0)
        down = [[None] * len(c) for c in down_cuts]
        down[0][0] = tp_swap(w_down, 0, *down_cuts[0][0])
        gate1 = tp_swap(w_gate, 1)
        for n, (lo, hi) in list(enumerate(up1_cuts))[1:]:
            up1[n] = tp_swap(w_up, 1, lo, hi)
        for k, n in late:
            lo, hi = down_cuts[k][n]
            down[k][n] = tp_swap(w_down, k, lo, hi)

        pos, gate, cap = routing(jnp.stack([ids_a, ids_b]), jnp.stack([gates_a, gates_b]), me)
        gate_t = gate.transpose(0, 2, 1)

        xs = []
        for b, tokens in enumerate((tokens_a, tokens_b)):
            rows = pos[b][:, None, :]
            far = dispatch(rows[4:], tokens, cap)
            far = [ep_swap(far[0], 2), ep_swap(far[1], 3)]
            near = dispatch(rows[:4], tokens, cap)
            xs.append([near[0], ep_swap(near[1], 1), *far])
        slots = jnp.arange(cap, dtype=jnp.int32)
        picks = [(pos.reshape(2, MASKS, 2, -1)[:, :, k, :, None] == slots).astype(BF16) for k in range(2)]

        p, h_l = None, []
        for b in range(2):
            h_l.append(hidden_local(xs[b], w_gate, w_up))
        for b in range(2):
            p = part(h_l[b], b, w_down, p)

        h_r = [None, None]
        for b in range(2):
            h_r[0] = hidden(xs[b], b, 0, gate0, up0, 0, h_r[0])
        for n, (lo, hi) in enumerate(up1_cuts):
            for b in range(2):
                h_r[1] = hidden(xs[b], b, 1, gate1, up1[n], lo, h_r[1])

        acc, outs = None, None
        for k, n in [(0, 0)] + late:
            lo, hi = down_cuts[k][n]
            if (k, n) in halves:
                far = final(h_r[k], p, k, down[k][n], lo, (2, 3))
                near = final(h_r[k], p, k, down[k][n], lo, (0, 1))
            else:
                *near, y2, y3 = final(h_r[k], p, k, down[k][n], lo, (0, 1, 2, 3))
                far = [y2, y3]
            far = [ep_swap(far[0], 2), ep_swap(far[1], 3)]
            near = [near[0], ep_swap(near[1], 1)]
            if k == 0:
                acc = combine(near + far, picks[0], gate_t, 0, lo, model, None, acc)
            else:
                outs = combine(near + far, picks[1], gate_t, 1, lo, model, acc, outs)
        return tuple(outs)

    in_specs = (row_spec, row_spec, row_spec, row_spec, row_spec, row_spec, gate_spec, gate_spec, down_spec)
    return jax.shard_map(group_body, mesh=mesh, in_specs=in_specs, out_specs=(row_spec, row_spec), check_vma=False)
```

```python
import functools

import jax
import jax.numpy as jnp
from jax import lax
from jax.experimental import pallas as pl
from jax.experimental.pallas import tpu as pltpu
from jax.sharding import PartitionSpec as P


TP_SWAP = [(0, 1), (1, 0)]
BF16 = jnp.bfloat16
F32 = jnp.float32
MASKS = 4
TN = 256
TB = 512
VMEM_LIMIT = 60 * 1024 * 1024


def mm(a, b):
    return jnp.dot(a, b, preferred_element_type=F32)


def call(kernel, flops, nbytes, **kw):
    params = pltpu.CompilerParams(vmem_limit_bytes=VMEM_LIMIT)
    cost = pl.CostEstimate(flops=int(flops), bytes_accessed=int(nbytes), transcendentals=0)
    return pl.pallas_call(kernel, compiler_params=params, cost_estimate=cost, **kw)


def filled_further(into, args, in_specs):
    if into is None:
        return {}
    args.append(into)
    in_specs.append(pl.BlockSpec(memory_space=pl.ANY))
    return {"input_output_aliases": {len(args) - 1: 0}}


def dispatch_kernel(pos_ref, tok_ref, *outs):
    step = pl.program_id(0)
    cap, model = outs[0].shape[1:]
    slots = lax.broadcasted_iota(jnp.int32, (cap, tok_ref.shape[0]), 0)
    onehot = (slots == pos_ref[0]).astype(BF16)
    for lo in range(0, model, 512):
        rows = mm(onehot, tok_ref[:, lo:lo + 512]).astype(BF16)
        for m, out in enumerate(outs):

            @pl.when(step // 2 == m)
            def _():
                out[0, :, lo:lo + 512] = rows


def dispatch(pos, tokens, cap):
    n = pos.shape[0] // 2
    toks, model = tokens.shape
    out = jax.ShapeDtypeStruct((2, cap, model), BF16)
    return call(
        dispatch_kernel, 2 * n * 2 * cap * toks * model, toks * model * 2 + 2 * n * cap * model * 2,
        grid=(2 * n,),
        in_specs=[pl.BlockSpec((1, 1, toks), lambda i: (i, 0, 0)), pl.BlockSpec((toks, model), lambda i: (0, 0))],
        out_specs=[pl.BlockSpec((1, cap, model), functools.partial(lambda m, i: (jnp.clip(i - 2 * m, 0, 1), 0, 0), m)) for m in range(n)],
        out_shape=[out] * n,
    )(pos, tokens)


def hidden_kernel(*refs):
    xs, (wg, wu), h = refs[:MASKS], refs[MASKS:MASKS + 2], refs[-1]
    g = wg[...].reshape(wg.shape[-2:])
    u = wu[...].reshape(wu.shape[-2:])
    for m in range(MASKS):
        x = xs[m][0]
        a = mm(x, g)
        h[0, m] = (a * jax.nn.sigmoid(a) * mm(x, u)).astype(BF16)


def hidden_local(xs, wg, wu):
    _, cap, model = xs[0].shape
    width = wg.shape[2]
    rows = 2 * MASKS * cap
    return call(
        hidden_kernel, 4 * rows * model * width, 2 * (rows * model + 4 * model * width + rows * width),
        grid=(2, width // TN),
        in_specs=[pl.BlockSpec((1, cap, model), lambda k, n: (k, 0, 0)) for _ in xs]
        + [pl.BlockSpec((1, model, TN), lambda k, n: (k, 0, n))] * 2,
        out_specs=pl.BlockSpec((1, MASKS, cap, TN), lambda k, n: (k, 0, 0, n)),
        out_shape=jax.ShapeDtypeStruct((2, MASKS, cap, width), BF16),
    )(*xs, wg, wu)


def hidden(xs, b, k, wg, wu, lo, into):
    _, cap, model = xs[0].shape
    width, cols = wg.shape[1], wu.shape[1]
    off, steps = lo // TN, cols // TN
    in_specs = [pl.BlockSpec((1, cap, model), lambda n: (k, 0, 0)) for _ in xs]
    in_specs += [pl.BlockSpec((model, TN), lambda n: (0, n + off)), pl.BlockSpec((model, TN), lambda n: (0, n))]
    args = [*xs, wg, wu]
    kw = filled_further(into, args, in_specs)
    rows = MASKS * cap
    return call(
        hidden_kernel, 4 * rows * model * cols, 2 * (rows * model + 2 * model * cols + rows * cols),
        grid=(steps,), in_specs=in_specs,
        out_specs=pl.BlockSpec((1, MASKS, cap, TN), lambda n: (b, 0, 0, n + off)),
        out_shape=jax.ShapeDtypeStruct((2, MASKS, cap, width), BF16), **kw,
    )(*args)


def part_kernel(h, wd, *refs):
    for m in range(MASKS):
        refs[-1][0, 0, m] = mm(h[0, m], wd[0])


def part(h, b, wd, into):
    _, _, cap, width = h.shape
    model = wd.shape[2]
    rows = 2 * MASKS * cap
    in_specs = [pl.BlockSpec((1, MASKS, cap, width), lambda k, n: (k, 0, 0, 0)), pl.BlockSpec((1, width, TN), lambda k, n: (k, 0, n))]
    args = [h, wd]
    kw = filled_further(into, args, in_specs)
    return call(
        part_kernel, 2 * rows * width * model, 2 * (rows * width + 2 * width * model) + 4 * rows * model,
        grid=(2, model // TN), in_specs=in_specs,
        out_specs=pl.BlockSpec((1, 1, MASKS, cap, TN), lambda k, n: (k, b, 0, 0, n)),
        out_shape=jax.ShapeDtypeStruct((2, 2, MASKS, cap, model), F32), **kw,
    )(*args)


def final_kernel(h0, h1, p, wd, *outs):
    m = pl.program_id(0) % len(outs)
    half = h0.shape[3]
    for j, h in enumerate((h0, h1)):
        rows = slice(j * half, (j + 1) * half)
        y = (p[0, 0, 0, rows] + mm(h[0, 0, 0], wd[...])).astype(BF16)
        for t, out in enumerate(outs):

            @pl.when(m == t)
            def _():
                out[0, rows] = y


def final(h, p, k, wd, lo, masks):
    _, _, cap, width = h.shape
    cols = wd.shape[1]
    at, n, m0 = lo // cols, len(masks), masks[0]
    rows = 2 * n * cap
    halves = h.reshape(2, MASKS, 2, cap // 2, width)
    return call(
        final_kernel, 2 * rows * width * cols, 2 * (rows * width + width * cols) + 6 * rows * cols,
        grid=(2 * n,),
        in_specs=[pl.BlockSpec((1, 1, 1, cap // 2, width), functools.partial(lambda j, i: (i // n, m0 + i % n, j, 0, 0), j)) for j in range(2)]
        + [
            pl.BlockSpec((1, 1, 1, cap, cols), lambda i: (k, i // n, m0 + i % n, 0, at)),
            pl.BlockSpec((width, cols), lambda i: (0, 0)),
        ],
        out_specs=[pl.BlockSpec((1, cap, cols), functools.partial(lambda m, i: (jnp.where(i >= n + m, 1, 0), 0, 0), m)) for m in range(n)],
        out_shape=[jax.ShapeDtypeStruct((2, cap, cols), BF16)] * n,
    )(halves, halves, p, wd)


def picked(k, groups, pos, gate):
    slots = lax.broadcasted_iota(jnp.int32, (TB, groups[0][0].shape[1]), 1)
    totals = [None] * len(groups)
    for m in range(MASKS):
        e = 2 * m + k
        onehot = (slots == pos[0, :, e:e + 1]).astype(BF16)
        for j, ys in enumerate(groups):
            term = gate[0, :, e:e + 1] * mm(onehot, ys[m][0])
            totals[j] = term if totals[j] is None else totals[j] + term
    return totals


def combine_kernel(k, n, *refs):
    groups = [refs[MASKS * j:MASKS * (j + 1)] for j in range(n)]
    totals = picked(k, groups, *refs[MASKS * n:MASKS * n + 2])
    cols = groups[0][0].shape[2]
    i, blocks = pl.program_id(0), pl.num_programs(0) // 2
    for j, total in enumerate(totals):
        at = slice(j * cols, (j + 1) * cols)
        if k == 0:
            refs[-1][:, at] = total
            continue
        total = (refs[MASKS * n + 2][:, at] + total).astype(BF16)
        for b, out in enumerate(refs[-2:]):

            @pl.when(i // blocks == b)
            def _():
                out[:, at] = total


def combine(groups, pos, gate, k, lo, model, acc=None, into=None):
    _, cap, cols = groups[0][0].shape
    n, wide = len(groups), cols * len(groups)
    toks = pos.shape[1]
    blocks = toks // TB
    at = lo // wide
    args = [y for ys in groups for y in ys] + [pos, gate]
    in_specs = [pl.BlockSpec((1, cap, cols), lambda i: (i // blocks, 0, 0))] * (MASKS * n)
    in_specs += [pl.BlockSpec((1, TB, pos.shape[2]), lambda i: (i // blocks, i % blocks, 0))] * 2
    flops, nbytes = 2 * 2 * toks * MASKS * cap * wide, 2 * toks * wide * 6
    kernel = functools.partial(combine_kernel, k, n)
    if k == 0:
        kw = filled_further(into, args, in_specs)
        return call(
            kernel, flops, nbytes,
            grid=(2 * blocks,), in_specs=in_specs,
            out_specs=pl.BlockSpec((TB, wide), lambda i: (i, at)),
            out_shape=jax.ShapeDtypeStruct((2 * toks, model), F32), **kw,
        )(*args)
    args.append(acc)
    in_specs.append(pl.BlockSpec((TB, wide), lambda i: (i, at)))
    kw = {}
    if into is not None:
        kw["input_output_aliases"] = {len(args): 0, len(args) + 1: 1}
        args += into
        in_specs += [pl.BlockSpec(memory_space=pl.ANY)] * 2
    return call(
        kernel, flops, nbytes,
        grid=(2 * blocks,), in_specs=in_specs,
        out_specs=[
            pl.BlockSpec((TB, wide), lambda i: (jnp.minimum(i, blocks - 1), at)),
            pl.BlockSpec((TB, wide), lambda i: (jnp.maximum(i - blocks, 0), at)),
        ],
        out_shape=[jax.ShapeDtypeStruct((toks, model), BF16)] * 2, **kw,
    )(*args)


def cuts(sizes):
    out, at = [], 0
    for size in sizes:
        out.append((at, at + size))
        at += size
    return out


def solution(mesh):
    ep_size = mesh.shape["ep"]
    row_spec = P(("dp", "ep", "tp"), None)
    gate_spec = P("ep", None, "tp")
    down_spec = P("ep", "tp", None)
    up1_cuts = cuts([512, 1024, 1024, 256])
    down_cuts = [cuts([1024] + [256] * 4), cuts([256] * 7 + [128, 128])]
    late = [(0, n) for n in range(1, 5)] + [(1, n) for n in range(9)]
    halves = [(1, 7), (1, 8)]
    groups = [[(0, 0)], [(0, 1), (0, 2)], [(0, 3), (0, 4)], [(1, 0), (1, 1)], [(1, 2), (1, 3)], [(1, 4), (1, 5)], [(1, 6)], [(1, 7)], [(1, 8)]]

    def ep_swap(value, mask):
        return lax.ppermute(value, "ep", [(i, i ^ mask) for i in range(ep_size)])

    def tp_swap(w, k, lo=0, hi=None):
        piece = lax.slice(w, (k, 0, lo), (k + 1, w.shape[1], w.shape[2] if hi is None else hi))
        return lax.ppermute(piece, "tp", TP_SWAP)[0]

    def routing(ids, gates, me):
        toks, top_k = ids.shape[1:]
        n_exp = 2 * ep_size
        mean_load = top_k * toks // n_exp
        cap = mean_load + mean_load // 4
        code = ((ids // 2) ^ me) * 2 + ids % 2
        hit = code[:, None] == jnp.arange(n_exp, dtype=jnp.int32)[None, :, None, None]
        has = jnp.any(hit, axis=3)
        count = has.astype(jnp.int32)
        pos = jnp.cumsum(count, axis=2) - count
        pos = jnp.where(has & (pos < cap), pos, -1)
        gate = jnp.sum(jnp.where(hit, gates[:, None], 0.0), axis=3)
        return pos, gate, cap

    def group_body(tokens_a, ids_a, gates_a, tokens_b, ids_b, gates_b, w_gate, w_up, w_down):
        me = lax.axis_index("ep")
        model = w_down.shape[2]
        up1 = [None] * len(up1_cuts)
        up1[0] = tp_swap(w_up, 1, *up1_cuts[0])
        gate0 = tp_swap(w_gate, 0)
        up0 = tp_swap(w_up, 0)
        down = [[None] * len(c) for c in down_cuts]
        down[0][0] = tp_swap(w_down, 0, *down_cuts[0][0])
        gate1 = tp_swap(w_gate, 1)
        for n, (lo, hi) in list(enumerate(up1_cuts))[1:]:
            up1[n] = tp_swap(w_up, 1, lo, hi)
        for k, n in late:
            lo, hi = down_cuts[k][n]
            down[k][n] = tp_swap(w_down, k, lo, hi)

        pos, gate, cap = routing(jnp.stack([ids_a, ids_b]), jnp.stack([gates_a, gates_b]), me)
        pos_t, gate_t = pos.transpose(0, 2, 1), gate.transpose(0, 2, 1)

        xs = []
        for b, tokens in enumerate((tokens_a, tokens_b)):
            rows = pos[b][:, None, :]
            far = dispatch(rows[4:], tokens, cap)
            far = [ep_swap(far[0], 2), ep_swap(far[1], 3)]
            near = dispatch(rows[:4], tokens, cap)
            xs.append([near[0], ep_swap(near[1], 1), *far])
        p, h_l = None, []
        for b in range(2):
            h_l.append(hidden_local(xs[b], w_gate, w_up))
        for b in range(2):
            p = part(h_l[b], b, w_down, p)

        h_r = [None, None]
        for b in range(2):
            h_r[0] = hidden(xs[b], b, 0, gate0, up0, 0, h_r[0])
        for n, (lo, hi) in enumerate(up1_cuts):
            for b in range(2):
                h_r[1] = hidden(xs[b], b, 1, gate1, up1[n], lo, h_r[1])

        acc, outs, back = None, None, {}
        for k, n in [(0, 0)] + late:
            lo, hi = down_cuts[k][n]
            if (k, n) in halves:
                far = final(h_r[k], p, k, down[k][n], lo, (2, 3))
                near = final(h_r[k], p, k, down[k][n], lo, (0, 1))
            else:
                *near, y2, y3 = final(h_r[k], p, k, down[k][n], lo, (0, 1, 2, 3))
                far = [y2, y3]
            far = [ep_swap(far[0], 2), ep_swap(far[1], 3)]
            near = [near[0], ep_swap(near[1], 1)]
            back[k, n] = near + far
        for group in groups:
            k, n = group[-1]
            lo = down_cuts[k][group[0][1]][0]
            done = [back[item] for item in group]
            if k == 0:
                acc = combine(done, pos_t, gate_t, 0, lo, model, None, acc)
            else:
                outs = combine(done, pos_t, gate_t, 1, lo, model, acc, outs)
        return tuple(outs)

    in_specs = (row_spec, row_spec, row_spec, row_spec, row_spec, row_spec, gate_spec, gate_spec, down_spec)
    return jax.shard_map(group_body, mesh=mesh, in_specs=in_specs, out_specs=(row_spec, row_spec), check_vma=False)
```

```python
import functools

import jax
import jax.numpy as jnp
from jax import lax
from jax.experimental import pallas as pl
from jax.experimental.pallas import tpu as pltpu
from jax.sharding import PartitionSpec as P


TP_SWAP = [(0, 1), (1, 0)]
BF16 = jnp.bfloat16
F32 = jnp.float32
MASKS = 4
TN = 256
TB = 512


def mm(a, b):
    return jnp.dot(a, b, preferred_element_type=F32)


def call(kernel, flops, nbytes, limit=60, **kw):
    params = pltpu.CompilerParams(vmem_limit_bytes=limit * 1024 * 1024)
    cost = pl.CostEstimate(flops=int(flops), bytes_accessed=int(nbytes), transcendentals=0)
    return pl.pallas_call(kernel, compiler_params=params, cost_estimate=cost, **kw)


def filled_further(into, args, in_specs):
    if into is None:
        return {}
    args.append(into)
    in_specs.append(pl.BlockSpec(memory_space=pl.ANY))
    return {"input_output_aliases": {len(args) - 1: 0}}


def kept(value, args, in_specs, output):
    args.append(pltpu.with_memory_space_constraint(value, pltpu.VMEM))
    in_specs.append(pl.BlockSpec(memory_space=pltpu.VMEM))
    return {"input_output_aliases": {len(args) - 1: output}}


def dispatch_kernel(pos_ref, tok_ref, *outs):
    step = pl.program_id(0)
    cap, model = outs[0].shape[1:]
    slots = lax.broadcasted_iota(jnp.int32, (cap, tok_ref.shape[0]), 0)
    onehot = (slots == pos_ref[0]).astype(BF16)
    for lo in range(0, model, 512):
        rows = mm(onehot, tok_ref[:, lo:lo + 512]).astype(BF16)
        for m, out in enumerate(outs):

            @pl.when(step // 2 == m)
            def _():
                out[0, :, lo:lo + 512] = rows


def dispatch(pos, tokens, cap):
    n = pos.shape[0] // 2
    toks, model = tokens.shape
    out = jax.ShapeDtypeStruct((2, cap, model), BF16)
    return call(
        dispatch_kernel, 2 * n * 2 * cap * toks * model, toks * model * 2 + 2 * n * cap * model * 2,
        grid=(2 * n,),
        in_specs=[pl.BlockSpec((1, 1, toks), lambda i: (i, 0, 0)), pl.BlockSpec((toks, model), lambda i: (0, 0))],
        out_specs=[pl.BlockSpec((1, cap, model), functools.partial(lambda m, i: (jnp.clip(i - 2 * m, 0, 1), 0, 0), m)) for m in range(n)],
        out_shape=[out] * n,
    )(pos, tokens)


def hidden_kernel(b, off, *refs):
    xs, (wg, wu), h = refs[:MASKS], refs[MASKS:MASKS + 2], refs[-1]
    g = wg[...].reshape(wg.shape[-2:])
    u = wu[...].reshape(wu.shape[-2:])
    for m in range(MASKS):
        x = xs[m][0]
        a = mm(x, g)
        out = (a * jax.nn.sigmoid(a) * mm(x, u)).astype(BF16)
        if b is None:
            h[0, m] = out
        else:
            h[b, m, :, pl.ds(pl.multiple_of((off + pl.program_id(0)) * TN, TN), TN)] = out


def hidden_local(xs, wg, wu):
    _, cap, model = xs[0].shape
    width = wg.shape[2]
    rows = 2 * MASKS * cap
    return call(
        functools.partial(hidden_kernel, None, 0), 4 * rows * model * width, 2 * (rows * model + 4 * model * width + rows * width),
        grid=(2, width // TN),
        in_specs=[pl.BlockSpec((1, cap, model), lambda k, n: (k, 0, 0)) for _ in xs]
        + [pl.BlockSpec((1, model, TN), lambda k, n: (k, 0, n))] * 2,
        out_specs=pl.BlockSpec((1, MASKS, cap, TN), lambda k, n: (k, 0, 0, n)),
        out_shape=jax.ShapeDtypeStruct((2, MASKS, cap, width), BF16),
    )(*xs, wg, wu)


def hidden(xs, b, k, wg, wu, lo, into):
    _, cap, model = xs[0].shape
    width, cols = wg.shape[1], wu.shape[1]
    off, steps = lo // TN, cols // TN
    in_specs = [pl.BlockSpec((1, cap, model), lambda n: (k, 0, 0)) for _ in xs]
    in_specs += [pl.BlockSpec((model, TN), lambda n: (0, n + off)), pl.BlockSpec((model, TN), lambda n: (0, n))]
    args = [*xs, wg, wu]
    rows = MASKS * cap
    cost = (4 * rows * model * cols, 2 * (rows * model + 2 * model * cols + rows * cols))
    if k == 1:
        kw = {}
        if into is not None:
            kw = kept(into, args, in_specs, 0)
        return call(
            functools.partial(hidden_kernel, b, off), *cost, 33,
            grid=(steps,), in_specs=in_specs,
            out_specs=pl.BlockSpec(memory_space=pltpu.VMEM),
            out_shape=pltpu.VMEM((2, MASKS, cap, width), BF16), **kw,
        )(*args)
    kw = filled_further(into, args, in_specs)
    return call(
        functools.partial(hidden_kernel, None, 0), *cost,
        grid=(steps,), in_specs=in_specs,
        out_specs=pl.BlockSpec((1, MASKS, cap, TN), lambda n: (b, 0, 0, n + off)),
        out_shape=jax.ShapeDtypeStruct((2, MASKS, cap, width), BF16), **kw,
    )(*args)


def part_kernel(h, wd, *refs):
    for m in range(MASKS):
        refs[-1][0, 0, m] = mm(h[0, m], wd[0])


def part(h, b, wd, into):
    _, _, cap, width = h.shape
    model = wd.shape[2]
    rows = 2 * MASKS * cap
    in_specs = [pl.BlockSpec((1, MASKS, cap, width), lambda k, n: (k, 0, 0, 0)), pl.BlockSpec((1, width, TN), lambda k, n: (k, 0, n))]
    args = [h, wd]
    kw = filled_further(into, args, in_specs)
    return call(
        part_kernel, 2 * rows * width * model, 2 * (rows * width + 2 * width * model) + 4 * rows * model,
        grid=(2, model // TN), in_specs=in_specs,
        out_specs=pl.BlockSpec((1, 1, MASKS, cap, TN), lambda k, n: (k, b, 0, 0, n)),
        out_shape=jax.ShapeDtypeStruct((2, 2, MASKS, cap, model), F32), **kw,
    )(*args)


def final_kernel(h0, h1, p, wd, *outs):
    q = pl.program_id(0) % 2
    for j, h in enumerate((h0, h1)):
        y = (p[0, 0, j] + mm(h[0, 0], wd[...])).astype(BF16)
        for t in range(2):

            @pl.when(q == t)
            def _():
                outs[2 * t + j][0] = y


def final(h, p, k, wd, lo):
    _, _, cap, width = h.shape
    cols = wd.shape[1]
    at = lo // cols
    rows = 2 * MASKS * cap
    return call(
        final_kernel, 2 * rows * width * cols, 2 * (rows * width + width * cols) + 6 * rows * cols, 57,
        grid=(4,),
        in_specs=[pl.BlockSpec((1, 1, cap, width), functools.partial(lambda j, i: (i // 2, 2 * (i % 2) + j, 0, 0), j)) for j in range(2)]
        + [
            pl.BlockSpec((1, 1, 2, cap, cols), lambda i: (k, i // 2, i % 2, 0, at)),
            pl.BlockSpec((width, cols), lambda i: (0, 0)),
        ],
        out_specs=[pl.BlockSpec((1, cap, cols), functools.partial(lambda m, i: (jnp.where(i >= 2 + m // 2, 1, 0), 0, 0), m)) for m in range(MASKS)],
        out_shape=[jax.ShapeDtypeStruct((2, cap, cols), BF16)] * MASKS,
    )(h, h, p, wd)


def final_kept_kernel(masks, p, wd, h, *refs):
    i, n = pl.program_id(0), len(masks)
    y = (p[0, 0, 0] + mm(h[i // n, masks[0] + i % n], wd[...])).astype(BF16)
    for j, out in enumerate(refs[:n]):

        @pl.when(i % n == j)
        def _():
            out[0] = y


def final_kept(h, p, k, wd, lo, masks):
    _, _, cap, width = h.shape
    cols = wd.shape[1]
    at, n, m0 = lo // cols, len(masks), masks[0]
    rows = 2 * n * cap
    args = [p, wd]
    in_specs = [
        pl.BlockSpec((1, 1, 1, cap, cols), lambda i: (k, i // n, m0 + i % n, 0, at)),
        pl.BlockSpec((width, cols), lambda i: (0, 0)),
    ]
    kw = kept(h, args, in_specs, n)
    return call(
        functools.partial(final_kept_kernel, masks), 2 * rows * width * cols, 6 * rows * cols, 33,
        grid=(2 * n,), in_specs=in_specs,
        out_specs=[pl.BlockSpec((1, cap, cols), functools.partial(lambda m, i: (jnp.where(i >= n + m, 1, 0), 0, 0), m)) for m in range(n)]
        + [pl.BlockSpec(memory_space=pltpu.VMEM)],
        out_shape=[jax.ShapeDtypeStruct((2, cap, cols), BF16)] * n + [pltpu.VMEM(h.shape, BF16)], **kw,
    )(*args)


def picked(k, groups, pos, gate):
    slots = lax.broadcasted_iota(jnp.int32, (TB, groups[0][0].shape[1]), 1)
    totals = [None] * len(groups)
    for m in range(MASKS):
        e = 2 * m + k
        onehot = (slots == pos[0, :, e:e + 1]).astype(BF16)
        for j, ys in enumerate(groups):
            term = gate[0, :, e:e + 1] * mm(onehot, ys[m][0])
            totals[j] = term if totals[j] is None else totals[j] + term
    return totals


def combine_kernel(k, n, held, *refs):
    if held:
        refs = refs[:-1]
    groups = [refs[MASKS * j:MASKS * (j + 1)] for j in range(n)]
    totals = picked(k, groups, *refs[MASKS * n:MASKS * n + 2])
    cols = groups[0][0].shape[2]
    i, blocks = pl.program_id(0), pl.num_programs(0) // 2
    for j, total in enumerate(totals):
        at = slice(j * cols, (j + 1) * cols)
        if k == 0:
            refs[-1][:, at] = total
            continue
        total = (refs[MASKS * n + 2][:, at] + total).astype(BF16)
        for b, out in enumerate(refs[-2:]):

            @pl.when(i // blocks == b)
            def _():
                out[:, at] = total


def combine(groups, pos, gate, k, lo, model, acc=None, into=None, held=None):
    _, cap, cols = groups[0][0].shape
    n, wide = len(groups), cols * len(groups)
    toks = pos.shape[1]
    blocks = toks // TB
    at = lo // wide
    args = [y for ys in groups for y in ys] + [pos, gate]
    in_specs = [pl.BlockSpec((1, cap, cols), lambda i: (i // blocks, 0, 0))] * (MASKS * n)
    in_specs += [pl.BlockSpec((1, TB, pos.shape[2]), lambda i: (i // blocks, i % blocks, 0))] * 2
    flops, nbytes = 2 * 2 * toks * MASKS * cap * wide, 2 * toks * wide * 6
    kernel = functools.partial(combine_kernel, k, n, held is not None)
    if k == 0:
        kw = filled_further(into, args, in_specs)
        return call(
            kernel, flops, nbytes, 20,
            grid=(2 * blocks,), in_specs=in_specs,
            out_specs=pl.BlockSpec((TB, wide), lambda i: (i, at)),
            out_shape=jax.ShapeDtypeStruct((2 * toks, model), F32), **kw,
        )(*args)
    args.append(acc)
    in_specs.append(pl.BlockSpec((TB, wide), lambda i: (i, at)))
    aliases = {}
    if into is not None:
        aliases = {len(args): 0, len(args) + 1: 1}
        args += into
        in_specs += [pl.BlockSpec(memory_space=pl.ANY)] * 2
    if held is not None:
        aliases |= kept(held, args, in_specs, 2)["input_output_aliases"]
    return call(
        kernel, flops, nbytes, 33,
        grid=(2 * blocks,), in_specs=in_specs,
        out_specs=[
            pl.BlockSpec((TB, wide), lambda i: (jnp.minimum(i, blocks - 1), at)),
            pl.BlockSpec((TB, wide), lambda i: (jnp.maximum(i - blocks, 0), at)),
        ] + [pl.BlockSpec(memory_space=pltpu.VMEM)] * (held is not None),
        out_shape=[jax.ShapeDtypeStruct((toks, model), BF16)] * 2 + ([] if held is None else [pltpu.VMEM(held.shape, BF16)]),
        input_output_aliases=aliases,
    )(*args)


def cuts(sizes):
    out, at = [], 0
    for size in sizes:
        out.append((at, at + size))
        at += size
    return out


def solution(mesh):
    ep_size = mesh.shape["ep"]
    row_spec = P(("dp", "ep", "tp"), None)
    gate_spec = P("ep", None, "tp")
    down_spec = P("ep", "tp", None)
    up1_cuts = cuts([512, 1024, 1024, 256])
    down_cuts = [cuts([1024, 512, 512]), cuts([256] * 7 + [128, 128])]
    late = [(1, n) for n in range(9)]
    halves = [(1, 7), (1, 8)]
    after = {(1, 3): [[(1, 0), (1, 1)]], (1, 5): [[(1, 2), (1, 3)]], (1, 7): [[(1, 4), (1, 5)]], (1, 8): [[(1, 6)], [(1, 7)], [(1, 8)]]}

    def ep_swap(value, mask):
        return lax.ppermute(value, "ep", [(i, i ^ mask) for i in range(ep_size)])

    def tp_swap(w, k, lo=0, hi=None):
        piece = lax.slice(w, (k, 0, lo), (k + 1, w.shape[1], w.shape[2] if hi is None else hi))
        return lax.ppermute(piece, "tp", TP_SWAP)[0]

    def routing(ids, gates, me):
        toks, top_k = ids.shape[1:]
        n_exp = 2 * ep_size
        mean_load = top_k * toks // n_exp
        cap = mean_load + mean_load // 4
        code = ((ids // 2) ^ me) * 2 + ids % 2
        hit = code[:, None] == jnp.arange(n_exp, dtype=jnp.int32)[None, :, None, None]
        has = jnp.any(hit, axis=3)
        count = has.astype(jnp.int32)
        pos = jnp.cumsum(count, axis=2) - count
        pos = jnp.where(has & (pos < cap), pos, -1)
        gate = jnp.sum(jnp.where(hit, gates[:, None], 0.0), axis=3)
        return pos, gate, cap

    def group_body(tokens_a, ids_a, gates_a, tokens_b, ids_b, gates_b, w_gate, w_up, w_down):
        me = lax.axis_index("ep")
        model = w_down.shape[2]
        up1 = [None] * len(up1_cuts)
        up1[0] = tp_swap(w_up, 1, *up1_cuts[0])
        gate0 = tp_swap(w_gate, 0)
        up0 = tp_swap(w_up, 0)
        down = [[None] * len(c) for c in down_cuts]
        for n, (lo, hi) in enumerate(down_cuts[0]):
            down[0][n] = tp_swap(w_down, 0, lo, hi)
        gate1 = tp_swap(w_gate, 1)
        for n, (lo, hi) in list(enumerate(up1_cuts))[1:]:
            up1[n] = tp_swap(w_up, 1, lo, hi)
        for k, n in late:
            lo, hi = down_cuts[k][n]
            down[k][n] = tp_swap(w_down, k, lo, hi)

        pos, gate, cap = routing(jnp.stack([ids_a, ids_b]), jnp.stack([gates_a, gates_b]), me)
        pos_t, gate_t = pos.transpose(0, 2, 1), gate.transpose(0, 2, 1)

        xs = []
        for b, tokens in enumerate((tokens_a, tokens_b)):
            rows = pos[b][:, None, :]
            far = dispatch(rows[4:], tokens, cap)
            far = [ep_swap(far[0], 2), ep_swap(far[1], 3)]
            near = dispatch(rows[:4], tokens, cap)
            xs.append([near[0], ep_swap(near[1], 1), *far])
        p, h_l = None, []
        for b in range(2):
            h_l.append(hidden_local(xs[b], w_gate, w_up))
        for b in range(2):
            p = part(h_l[b], b, w_down, p)

        h_r = [None, None]
        for b in range(2):
            h_r[0] = hidden(xs[b], b, 0, gate0, up0, 0, h_r[0])
        for n, (lo, hi) in enumerate(up1_cuts):
            for b in range(2):
                h_r[1] = hidden(xs[b], b, 1, gate1, up1[n], lo, h_r[1])

        acc, outs, back = None, None, {}

        def finish(k, n):
            lo, _ = down_cuts[k][n]
            if (k, n) in halves:
                *far, h_r[k] = final_kept(h_r[k], p, k, down[k][n], lo, (2, 3))
                *near, h_r[k] = final_kept(h_r[k], p, k, down[k][n], lo, (0, 1))
            else:
                if k == 0:
                    ys = final(h_r[k], p, k, down[k][n], lo)
                else:
                    *ys, h_r[k] = final_kept(h_r[k], p, k, down[k][n], lo, (0, 1, 2, 3))
                near, far = ys[:2], ys[2:]
            far = [ep_swap(far[0], 2), ep_swap(far[1], 3)]
            near = [near[0], ep_swap(near[1], 1)]
            back[k, n] = near + far

        for item in (0, 0), (0, 1), (0, 2):
            finish(*item)
            acc = combine([back[item]], pos_t, gate_t, 0, down_cuts[0][item[1]][0], model, None, acc)
        for i, item in enumerate(late):
            finish(*item)
            for group in after.get(item, []):
                outs = combine(
                    [back[it] for it in group], pos_t, gate_t, 1, down_cuts[1][group[0][1]][0], model, acc, outs,
                    h_r[1] if i < len(late) - 1 else None,
                )
                if i < len(late) - 1:
                    *outs, h_r[1] = outs
        return tuple(outs)

    in_specs = (row_spec, row_spec, row_spec, row_spec, row_spec, row_spec, gate_spec, gate_spec, down_spec)
    return jax.shard_map(group_body, mesh=mesh, in_specs=in_specs, out_specs=(row_spec, row_spec), check_vma=False)
```

```python
import functools

import jax
import jax.numpy as jnp
from jax import lax
from jax.experimental import pallas as pl
from jax.experimental.pallas import tpu as pltpu
from jax.sharding import PartitionSpec as P


TP_SWAP = [(0, 1), (1, 0)]
BF16 = jnp.bfloat16
F32 = jnp.float32
MASKS = 4
TN = 256
TB = 512
WIN = 256


def mm(a, b):
    return jnp.dot(a, b, preferred_element_type=F32)


def call(kernel, flops, nbytes, limit=60, **kw):
    params = pltpu.CompilerParams(vmem_limit_bytes=limit * 1024 * 1024)
    cost = pl.CostEstimate(flops=int(flops), bytes_accessed=int(nbytes), transcendentals=0)
    return pl.pallas_call(kernel, compiler_params=params, cost_estimate=cost, **kw)


def filled_further(into, args, in_specs):
    if into is None:
        return {}
    args.append(into)
    in_specs.append(pl.BlockSpec(memory_space=pl.ANY))
    return {"input_output_aliases": {len(args) - 1: 0}}


def kept(value, args, in_specs, output):
    args.append(pltpu.with_memory_space_constraint(value, pltpu.VMEM))
    in_specs.append(pl.BlockSpec(memory_space=pltpu.VMEM))
    return {"input_output_aliases": {len(args) - 1: output}}


def dispatch_kernel(pos_ref, tok_ref, *outs):
    step = pl.program_id(0)
    cap, model = outs[0].shape[1:]
    slots = lax.broadcasted_iota(jnp.int32, (cap, tok_ref.shape[0]), 0)
    onehot = (slots == pos_ref[0]).astype(BF16)
    for lo in range(0, model, 512):
        rows = mm(onehot, tok_ref[:, lo:lo + 512]).astype(BF16)
        for m, out in enumerate(outs):

            @pl.when(step // 2 == m)
            def _():
                out[0, :, lo:lo + 512] = rows


def dispatch(pos, tokens, cap):
    n = pos.shape[0] // 2
    toks, model = tokens.shape
    out = jax.ShapeDtypeStruct((2, cap, model), BF16)
    return call(
        dispatch_kernel, 2 * n * 2 * cap * toks * model, toks * model * 2 + 2 * n * cap * model * 2,
        grid=(2 * n,),
        in_specs=[pl.BlockSpec((1, 1, toks), lambda i: (i, 0, 0)), pl.BlockSpec((toks, model), lambda i: (0, 0))],
        out_specs=[pl.BlockSpec((1, cap, model), functools.partial(lambda m, i: (jnp.clip(i - 2 * m, 0, 1), 0, 0), m)) for m in range(n)],
        out_shape=[out] * n,
    )(pos, tokens)


def hidden_kernel(b, off, *refs):
    xs, (wg, wu), h = refs[:MASKS], refs[MASKS:MASKS + 2], refs[-1]
    g = wg[...].reshape(wg.shape[-2:])
    u = wu[...].reshape(wu.shape[-2:])
    for m in range(MASKS):
        x = xs[m][0]
        a = mm(x, g)
        out = (a * jax.nn.sigmoid(a) * mm(x, u)).astype(BF16)
        if b is None:
            h[0, m] = out
        else:
            h[b, m, :, pl.ds(pl.multiple_of((off + pl.program_id(0)) * TN, TN), TN)] = out


def hidden_local(xs, wg, wu):
    _, cap, model = xs[0].shape
    width = wg.shape[2]
    rows = 2 * MASKS * cap
    return call(
        functools.partial(hidden_kernel, None, 0), 4 * rows * model * width, 2 * (rows * model + 4 * model * width + rows * width),
        grid=(2, width // TN),
        in_specs=[pl.BlockSpec((1, cap, model), lambda k, n: (k, 0, 0)) for _ in xs]
        + [pl.BlockSpec((1, model, TN), lambda k, n: (k, 0, n))] * 2,
        out_specs=pl.BlockSpec((1, MASKS, cap, TN), lambda k, n: (k, 0, 0, n)),
        out_shape=jax.ShapeDtypeStruct((2, MASKS, cap, width), BF16),
    )(*xs, wg, wu)


def hidden(xs, b, k, wg, wu, lo, into):
    _, cap, model = xs[0].shape
    width, cols = wg.shape[1], wu.shape[1]
    off, steps = lo // TN, cols // TN
    in_specs = [pl.BlockSpec((1, cap, model), lambda n: (k, 0, 0)) for _ in xs]
    in_specs += [pl.BlockSpec((model, TN), lambda n: (0, n + off)), pl.BlockSpec((model, TN), lambda n: (0, n))]
    args = [*xs, wg, wu]
    rows = MASKS * cap
    cost = (4 * rows * model * cols, 2 * (rows * model + 2 * model * cols + rows * cols))
    if k == 1:
        kw = {}
        if into is not None:
            kw = kept(into, args, in_specs, 0)
        return call(
            functools.partial(hidden_kernel, b, off), *cost, 33,
            grid=(steps,), in_specs=in_specs,
            out_specs=pl.BlockSpec(memory_space=pltpu.VMEM),
            out_shape=pltpu.VMEM((2, MASKS, cap, width), BF16), **kw,
        )(*args)
    kw = filled_further(into, args, in_specs)
    return call(
        functools.partial(hidden_kernel, None, 0), *cost,
        grid=(steps,), in_specs=in_specs,
        out_specs=pl.BlockSpec((1, MASKS, cap, TN), lambda n: (b, 0, 0, n + off)),
        out_shape=jax.ShapeDtypeStruct((2, MASKS, cap, width), BF16), **kw,
    )(*args)


def part_kernel(h, wd, *refs):
    for m in range(MASKS):
        refs[-1][0, 0, m] = mm(h[0, m], wd[0])


def part(h, b, wd, into):
    _, _, cap, width = h.shape
    model = wd.shape[2]
    rows = 2 * MASKS * cap
    in_specs = [pl.BlockSpec((1, MASKS, cap, width), lambda k, n: (k, 0, 0, 0)), pl.BlockSpec((1, width, TN), lambda k, n: (k, 0, n))]
    args = [h, wd]
    kw = filled_further(into, args, in_specs)
    return call(
        part_kernel, 2 * rows * width * model, 2 * (rows * width + 2 * width * model) + 4 * rows * model,
        grid=(2, model // TN), in_specs=in_specs,
        out_specs=pl.BlockSpec((1, 1, MASKS, cap, TN), lambda k, n: (k, b, 0, 0, n)),
        out_shape=jax.ShapeDtypeStruct((2, 2, MASKS, cap, model), F32), **kw,
    )(*args)


def final_kernel(h0, h1, p, wd, *outs):
    q = pl.program_id(0) % 2
    for j, h in enumerate((h0, h1)):
        y = (p[0, 0, j] + mm(h[0, 0], wd[...])).astype(BF16)
        for t in range(2):

            @pl.when(q == t)
            def _():
                outs[2 * t + j][0] = y


def final(h, p, k, wd, lo):
    _, _, cap, width = h.shape
    cols = wd.shape[1]
    at = lo // cols
    rows = 2 * MASKS * cap
    return call(
        final_kernel, 2 * rows * width * cols, 2 * (rows * width + width * cols) + 6 * rows * cols, 57,
        grid=(4,),
        in_specs=[pl.BlockSpec((1, 1, cap, width), functools.partial(lambda j, i: (i // 2, 2 * (i % 2) + j, 0, 0), j)) for j in range(2)]
        + [
            pl.BlockSpec((1, 1, 2, cap, cols), lambda i: (k, i // 2, i % 2, 0, at)),
            pl.BlockSpec((width, cols), lambda i: (0, 0)),
        ],
        out_specs=[pl.BlockSpec((1, cap, cols), functools.partial(lambda m, i: (jnp.where(i >= 2 + m // 2, 1, 0), 0, 0), m)) for m in range(MASKS)],
        out_shape=[jax.ShapeDtypeStruct((2, cap, cols), BF16)] * MASKS,
    )(h, h, p, wd)


def final_kept_kernel(masks, p, wd, h, *refs):
    i = pl.program_id(0)
    per_batch = len(masks) // 2
    m = masks[0] + 2 * (i % per_batch)
    _, _, cap, width = h.shape
    rows = h[i // per_batch, pl.ds(m, 2)].reshape(2 * cap, width)
    y = (p[0, 0].reshape(2 * cap, -1) + mm(rows, wd[...])).astype(BF16)
    for q in range(per_batch):

        @pl.when(i % per_batch == q)
        def _():
            refs[2 * q][0] = y[:cap]
            refs[2 * q + 1][0] = y[cap:]


def final_kept(h, p, k, wd, lo, masks):
    _, _, cap, width = h.shape
    cols = wd.shape[1]
    at, n, m0 = lo // cols, len(masks), masks[0]
    steps = n // 2
    rows = 2 * n * cap
    args = [p, wd]
    in_specs = [
        pl.BlockSpec((1, 1, 2, cap, cols), lambda i: (k, i // steps, m0 // 2 + i % steps, 0, at)),
        pl.BlockSpec((width, cols), lambda i: (0, 0)),
    ]
    kw = kept(h, args, in_specs, n)
    return call(
        functools.partial(final_kept_kernel, masks), 2 * rows * width * cols, 6 * rows * cols, 33,
        grid=(n,), in_specs=in_specs,
        out_specs=[pl.BlockSpec((1, cap, cols), functools.partial(lambda q, i: (jnp.where(i >= steps + q, 1, 0), 0, 0), m // 2)) for m in range(n)]
        + [pl.BlockSpec(memory_space=pltpu.VMEM)],
        out_shape=[jax.ShapeDtypeStruct((2, cap, cols), BF16)] * n + [pltpu.VMEM(h.shape, BF16)], **kw,
    )(*args)


def picked(k, groups, pos, gate, lo):
    slots = lax.broadcasted_iota(jnp.int32, (TB, WIN), 1)
    totals = [None] * len(groups)
    for m in range(MASKS):
        e = 2 * m + k
        at = pl.multiple_of(lo[m], 16)
        onehot = (slots == pos[0, :, e:e + 1] - at).astype(BF16)
        for j, ys in enumerate(groups):
            term = gate[0, :, e:e + 1] * mm(onehot, ys[m][0, pl.ds(at, WIN)])
            totals[j] = term if totals[j] is None else totals[j] + term
    return totals


def combine_kernel(k, n, held, first, last, *refs):
    total = refs[-1]
    refs = refs[:-2] if held else refs[:-1]
    groups = [refs[MASKS * j:MASKS * (j + 1)] for j in range(n)]
    pos, gate = refs[MASKS * n:MASKS * n + 2]
    cap, cols = groups[0][0].shape[1:]
    i, blocks = pl.program_id(0), pl.num_programs(0) // 2
    begin = [(jnp.minimum(first[i * MASKS + m], cap - WIN) // 16) * 16 for m in range(MASKS)]
    for j, part in enumerate(picked(k, groups, pos, gate, begin)):
        total[:, j * cols:(j + 1) * cols] = part
    slots = lax.broadcasted_iota(jnp.int32, (TB, WIN), 1)
    for m in range(MASKS):
        e = 2 * m + k
        end = last[i * MASKS + m]

        @pl.when(end > begin[m] + WIN)
        def _():
            def more(step, carry):
                lo = begin[m] + WIN + step * WIN
                at = pl.multiple_of(jnp.minimum(lo, cap - WIN), 16)
                mine = pos[0, :, e:e + 1]
                onehot = (slots == jnp.where(mine >= lo, mine - at, -1)).astype(BF16)
                for j, ys in enumerate(groups):
                    total[:, j * cols:(j + 1) * cols] += gate[0, :, e:e + 1] * mm(onehot, ys[m][0, pl.ds(at, WIN)])
                return carry

            lax.fori_loop(0, (end - begin[m] - 1) // WIN, more, 0)

    if k == 0:
        refs[-1][...] = total[...]
        return
    result = (refs[MASKS * n + 2][...] + total[...]).astype(BF16)
    for b, out in enumerate(refs[-2:]):

        @pl.when(i // blocks == b)
        def _():
            out[...] = result


def combine(groups, table, k, lo, model, acc=None, into=None, held=None):
    pos, gate, first, last = table
    _, cap, cols = groups[0][0].shape
    n, wide = len(groups), cols * len(groups)
    toks = pos.shape[1]
    blocks = toks // TB
    at = lo // wide
    args = [first[k], last[k]] + [y for ys in groups for y in ys] + [pos, gate]
    in_specs = [pl.BlockSpec((1, cap, cols), lambda i, *_: (i // blocks, 0, 0))] * (MASKS * n)
    in_specs += [pl.BlockSpec((1, TB, pos.shape[2]), lambda i, *_: (i // blocks, i % blocks, 0))] * 2
    aliases = {}
    if k == 0:
        if into is not None:
            aliases |= filled_further(into, args, in_specs)["input_output_aliases"]
        out_specs = pl.BlockSpec((TB, wide), lambda i, *_: (i, at))
        out_shape = jax.ShapeDtypeStruct((2 * toks, model), F32)
    else:
        args.append(acc)
        in_specs.append(pl.BlockSpec((TB, wide), lambda i, *_: (i, at)))
        if into is not None:
            aliases = {len(args): 0, len(args) + 1: 1}
            args += into
            in_specs += [pl.BlockSpec(memory_space=pl.ANY)] * 2
        out_specs = [
            pl.BlockSpec((TB, wide), lambda i, *_: (jnp.minimum(i, blocks - 1), at)),
            pl.BlockSpec((TB, wide), lambda i, *_: (jnp.maximum(i - blocks, 0), at)),
        ]
        out_shape = [jax.ShapeDtypeStruct((toks, model), BF16)] * 2
        if held is not None:
            aliases |= kept(held, args, in_specs, 2)["input_output_aliases"]
            out_specs.append(pl.BlockSpec(memory_space=pltpu.VMEM))
            out_shape.append(pltpu.VMEM(held.shape, BF16))
    return call(
        functools.partial(combine_kernel, k, n, held is not None),
        2 * 2 * toks * MASKS * WIN * wide, 2 * toks * wide * 6, 33 if k else 20,
        grid_spec=pltpu.PrefetchScalarGridSpec(
            num_scalar_prefetch=2, grid=(2 * blocks,), in_specs=in_specs, out_specs=out_specs,
            scratch_shapes=[pltpu.VMEM((TB, wide), F32)],
        ),
        out_shape=out_shape, input_output_aliases=aliases,
    )(*args)


def cuts(sizes):
    out, at = [], 0
    for size in sizes:
        out.append((at, at + size))
        at += size
    return out


def solution(mesh):
    ep_size = mesh.shape["ep"]
    row_spec = P(("dp", "ep", "tp"), None)
    gate_spec = P("ep", None, "tp")
    down_spec = P("ep", "tp", None)
    up1_cuts = cuts([256, 1280, 768, 512])
    down_cuts = [cuts([1024, 512, 512]), cuts([256] * 7 + [128, 128])]
    late = [(1, n) for n in range(9)]
    halves = [(1, n) for n in range(5, 9)]
    after = {(1, 2): [[(1, 0), (1, 1)]], (1, 4): [[(1, 2)]], (1, 5): [[(1, 3)]], (1, 6): [[(1, 4), (1, 5)]]}
    after[1, 8] = [[(1, 6)], [(1, 7)], [(1, 8)]]

    def ep_swap(value, mask):
        return lax.ppermute(value, "ep", [(i, i ^ mask) for i in range(ep_size)])

    def tp_swap(w, k, lo=0, hi=None):
        piece = lax.slice(w, (k, 0, lo), (k + 1, w.shape[1], w.shape[2] if hi is None else hi))
        return lax.ppermute(piece, "tp", TP_SWAP)[0]

    def routing(ids, gates, me):
        toks, top_k = ids.shape[1:]
        n_exp = 2 * ep_size
        mean_load = top_k * toks // n_exp
        cap = mean_load + mean_load // 4
        code = ((ids // 2) ^ me) * 2 + ids % 2
        hit = code[:, None] == jnp.arange(n_exp, dtype=jnp.int32)[None, :, None, None]
        has = jnp.any(hit, axis=3)
        count = has.astype(jnp.int32)
        pos = jnp.cumsum(count, axis=2) - count
        pos = jnp.where(has & (pos < cap), pos, -1)
        gate = jnp.sum(jnp.where(hit, gates[:, None], 0.0), axis=3)
        used = jnp.sum(count.reshape(2, n_exp, toks // TB, TB), axis=3)
        upto = jnp.cumsum(used, axis=2)
        first, last = jnp.minimum(upto - used, cap), jnp.minimum(upto, cap)
        order = lambda a: a.reshape(2, ep_size, 2, toks // TB).transpose(2, 0, 3, 1).reshape(2, -1)
        return pos, gate, cap, order(first), order(last)

    def group_body(tokens_a, ids_a, gates_a, tokens_b, ids_b, gates_b, w_gate, w_up, w_down):
        me = lax.axis_index("ep")
        model = w_down.shape[2]
        up1 = [None] * len(up1_cuts)
        up1[0] = tp_swap(w_up, 1, *up1_cuts[0])
        gate0 = tp_swap(w_gate, 0)
        up0 = tp_swap(w_up, 0)
        down = [[None] * len(c) for c in down_cuts]
        for n, (lo, hi) in enumerate(down_cuts[0]):
            down[0][n] = tp_swap(w_down, 0, lo, hi)
        gate1 = tp_swap(w_gate, 1)
        for n, (lo, hi) in list(enumerate(up1_cuts))[1:]:
            up1[n] = tp_swap(w_up, 1, lo, hi)
        for k, n in late:
            lo, hi = down_cuts[k][n]
            down[k][n] = tp_swap(w_down, k, lo, hi)

        pos, gate, cap, first, last = routing(jnp.stack([ids_a, ids_b]), jnp.stack([gates_a, gates_b]), me)
        table = pos.transpose(0, 2, 1), gate.transpose(0, 2, 1), first, last

        xs = []
        for b, tokens in enumerate((tokens_a, tokens_b)):
            rows = pos[b][:, None, :]
            far = dispatch(rows[4:], tokens, cap)
            far = [ep_swap(far[0], 2), ep_swap(far[1], 3)]
            near = dispatch(rows[:4], tokens, cap)
            xs.append([near[0], ep_swap(near[1], 1), *far])
        p, h_l = None, []
        for b in range(2):
            h_l.append(hidden_local(xs[b], w_gate, w_up))
        for b in range(2):
            p = part(h_l[b], b, w_down, p)

        h_r = [None, None]
        for b in range(2):
            h_r[0] = hidden(xs[b], b, 0, gate0, up0, 0, h_r[0])
        for n, (lo, hi) in enumerate(up1_cuts):
            for b in range(2):
                h_r[1] = hidden(xs[b], b, 1, gate1, up1[n], lo, h_r[1])

        acc, outs, back = None, None, {}

        def finish(k, n):
            lo, _ = down_cuts[k][n]
            if (k, n) in halves:
                *far, h_r[k] = final_kept(h_r[k], p, k, down[k][n], lo, (2, 3))
                *near, h_r[k] = final_kept(h_r[k], p, k, down[k][n], lo, (0, 1))
            else:
                if k == 0:
                    ys = final(h_r[k], p, k, down[k][n], lo)
                else:
                    *ys, h_r[k] = final_kept(h_r[k], p, k, down[k][n], lo, (0, 1, 2, 3))
                near, far = ys[:2], ys[2:]
            far = [ep_swap(far[0], 2), ep_swap(far[1], 3)]
            near = [near[0], ep_swap(near[1], 1)]
            back[k, n] = near + far

        for item in (0, 0), (0, 1), (0, 2):
            finish(*item)
            acc = combine([back[item]], table, 0, down_cuts[0][item[1]][0], model, None, acc)
        for i, item in enumerate(late):
            finish(*item)
            for group in after.get(item, []):
                outs = combine(
                    [back[it] for it in group], table, 1, down_cuts[1][group[0][1]][0], model, acc, outs,
                    h_r[1] if i < len(late) - 1 else None,
                )
                if i < len(late) - 1:
                    *outs, h_r[1] = outs
        return tuple(outs)

    in_specs = (row_spec, row_spec, row_spec, row_spec, row_spec, row_spec, gate_spec, gate_spec, down_spec)
    return jax.shard_map(group_body, mesh=mesh, in_specs=in_specs, out_specs=(row_spec, row_spec), check_vma=False)
```

```python
import functools

import jax
import jax.numpy as jnp
from jax import lax
from jax.experimental import pallas as pl
from jax.experimental.pallas import tpu as pltpu
from jax.sharding import PartitionSpec as P


TP_SWAP = [(0, 1), (1, 0)]
BF16 = jnp.bfloat16
F32 = jnp.float32
MASKS = 4
TN = 256
TB = 512
WIN = 256
INFO = 128


def mm(a, b):
    return jnp.dot(a, b, preferred_element_type=F32)


def call(kernel, flops, nbytes, limit=60, **kw):
    params = pltpu.CompilerParams(vmem_limit_bytes=limit * 1024 * 1024)
    cost = pl.CostEstimate(flops=int(flops), bytes_accessed=int(nbytes), transcendentals=0)
    return pl.pallas_call(kernel, compiler_params=params, cost_estimate=cost, **kw)


def filled_further(into, args, in_specs):
    if into is None:
        return {}
    args.append(into)
    in_specs.append(pl.BlockSpec(memory_space=pl.ANY))
    return {"input_output_aliases": {len(args) - 1: 0}}


def kept(value, args, in_specs, output):
    args.append(pltpu.with_memory_space_constraint(value, pltpu.VMEM))
    in_specs.append(pl.BlockSpec(memory_space=pltpu.VMEM))
    return {"input_output_aliases": {len(args) - 1: output}}


def dispatch_kernel(pos_ref, tok_ref, *outs):
    step = pl.program_id(0)
    cap, model = outs[0].shape[1:]
    slots = lax.broadcasted_iota(jnp.int32, (cap, tok_ref.shape[0]), 0)
    onehot = (slots == pos_ref[0]).astype(BF16)
    for lo in range(0, model, 512):
        rows = mm(onehot, tok_ref[:, lo:lo + 512]).astype(BF16)
        for m, out in enumerate(outs):

            @pl.when(step // 2 == m)
            def _():
                out[0, :, lo:lo + 512] = rows


def dispatch(pos, tokens, cap):
    n = pos.shape[0] // 2
    toks, model = tokens.shape
    out = jax.ShapeDtypeStruct((2, cap, model), BF16)
    return call(
        dispatch_kernel, 2 * n * 2 * cap * toks * model, toks * model * 2 + 2 * n * cap * model * 2,
        grid=(2 * n,),
        in_specs=[pl.BlockSpec((1, 1, toks), lambda i: (i, 0, 0)), pl.BlockSpec((toks, model), lambda i: (0, 0))],
        out_specs=[pl.BlockSpec((1, cap, model), functools.partial(lambda m, i: (jnp.clip(i - 2 * m, 0, 1), 0, 0), m)) for m in range(n)],
        out_shape=[out] * n,
    )(pos, tokens)


def hidden_kernel(b, off, *refs):
    xs, (wg, wu), h = refs[:MASKS], refs[MASKS:MASKS + 2], refs[-1]
    g = wg[...].reshape(wg.shape[-2:])
    u = wu[...].reshape(wu.shape[-2:])
    for m in range(MASKS):
        x = xs[m][0]
        a = mm(x, g)
        out = (a * jax.nn.sigmoid(a) * mm(x, u)).astype(BF16)
        if b is None:
            h[0, m] = out
        else:
            h[b, m, :, pl.ds(pl.multiple_of((off + pl.program_id(0)) * TN, TN), TN)] = out


def hidden_local(xs, wg, wu):
    _, cap, model = xs[0].shape
    width = wg.shape[2]
    rows = 2 * MASKS * cap
    return call(
        functools.partial(hidden_kernel, None, 0), 4 * rows * model * width, 2 * (rows * model + 4 * model * width + rows * width),
        grid=(2, width // TN),
        in_specs=[pl.BlockSpec((1, cap, model), lambda k, n: (k, 0, 0)) for _ in xs]
        + [pl.BlockSpec((1, model, TN), lambda k, n: (k, 0, n))] * 2,
        out_specs=pl.BlockSpec((1, MASKS, cap, TN), lambda k, n: (k, 0, 0, n)),
        out_shape=jax.ShapeDtypeStruct((2, MASKS, cap, width), BF16),
    )(*xs, wg, wu)


def hidden(xs, b, k, wg, wu, lo, into):
    _, cap, model = xs[0].shape
    width, cols = wg.shape[1], wu.shape[1]
    off, steps = lo // TN, cols // TN
    in_specs = [pl.BlockSpec((1, cap, model), lambda n: (k, 0, 0)) for _ in xs]
    in_specs += [pl.BlockSpec((model, TN), lambda n: (0, n + off)), pl.BlockSpec((model, TN), lambda n: (0, n))]
    args = [*xs, wg, wu]
    rows = MASKS * cap
    cost = (4 * rows * model * cols, 2 * (rows * model + 2 * model * cols + rows * cols))
    if k == 1:
        kw = {}
        if into is not None:
            kw = kept(into, args, in_specs, 0)
        return call(
            functools.partial(hidden_kernel, b, off), *cost, 33,
            grid=(steps,), in_specs=in_specs,
            out_specs=pl.BlockSpec(memory_space=pltpu.VMEM),
            out_shape=pltpu.VMEM((2, MASKS, cap, width), BF16), **kw,
        )(*args)
    kw = filled_further(into, args, in_specs)
    return call(
        functools.partial(hidden_kernel, None, 0), *cost,
        grid=(steps,), in_specs=in_specs,
        out_specs=pl.BlockSpec((1, MASKS, cap, TN), lambda n: (b, 0, 0, n + off)),
        out_shape=jax.ShapeDtypeStruct((2, MASKS, cap, width), BF16), **kw,
    )(*args)


def part_kernel(h, wd, *refs):
    for m in range(MASKS):
        refs[-1][0, 0, m] = mm(h[0, m], wd[0])


def part(h, b, wd, into):
    _, _, cap, width = h.shape
    model = wd.shape[2]
    rows = 2 * MASKS * cap
    in_specs = [pl.BlockSpec((1, MASKS, cap, width), lambda k, n: (k, 0, 0, 0)), pl.BlockSpec((1, width, TN), lambda k, n: (k, 0, n))]
    args = [h, wd]
    kw = filled_further(into, args, in_specs)
    return call(
        part_kernel, 2 * rows * width * model, 2 * (rows * width + 2 * width * model) + 4 * rows * model,
        grid=(2, model // TN), in_specs=in_specs,
        out_specs=pl.BlockSpec((1, 1, MASKS, cap, TN), lambda k, n: (k, b, 0, 0, n)),
        out_shape=jax.ShapeDtypeStruct((2, 2, MASKS, cap, model), F32), **kw,
    )(*args)


def final_kernel(h0, h1, p, wd, *outs):
    q = pl.program_id(0) % 2
    for j, h in enumerate((h0, h1)):
        y = (p[0, 0, j] + mm(h[0, 0], wd[...])).astype(BF16)
        for t in range(2):

            @pl.when(q == t)
            def _():
                outs[2 * t + j][0] = y


def final(h, p, k, wd, lo):
    _, _, cap, width = h.shape
    cols = wd.shape[1]
    at = lo // cols
    rows = 2 * MASKS * cap
    return call(
        final_kernel, 2 * rows * width * cols, 2 * (rows * width + width * cols) + 6 * rows * cols, 57,
        grid=(4,),
        in_specs=[pl.BlockSpec((1, 1, cap, width), functools.partial(lambda j, i: (i // 2, 2 * (i % 2) + j, 0, 0), j)) for j in range(2)]
        + [
            pl.BlockSpec((1, 1, 2, cap, cols), lambda i: (k, i // 2, i % 2, 0, at)),
            pl.BlockSpec((width, cols), lambda i: (0, 0)),
        ],
        out_specs=[pl.BlockSpec((1, cap, cols), functools.partial(lambda m, i: (jnp.where(i >= 2 + m // 2, 1, 0), 0, 0), m)) for m in range(MASKS)],
        out_shape=[jax.ShapeDtypeStruct((2, cap, cols), BF16)] * MASKS,
    )(h, h, p, wd)


def final_kept_kernel(masks, p, wd, h, *refs):
    i = pl.program_id(0)
    per_batch = len(masks) // 2
    m = masks[0] + 2 * (i % per_batch)
    _, _, cap, width = h.shape
    rows = h[i // per_batch, pl.ds(m, 2)].reshape(2 * cap, width)
    y = (p[0, 0].reshape(2 * cap, -1) + mm(rows, wd[...])).astype(BF16)
    for q in range(per_batch):

        @pl.when(i % per_batch == q)
        def _():
            refs[2 * q][0] = y[:cap]
            refs[2 * q + 1][0] = y[cap:]


def final_kept(h, p, k, wd, lo, masks):
    _, _, cap, width = h.shape
    cols = wd.shape[1]
    at, n, m0 = lo // cols, len(masks), masks[0]
    steps = n // 2
    rows = 2 * n * cap
    args = [p, wd]
    in_specs = [
        pl.BlockSpec((1, 1, 2, cap, cols), lambda i: (k, i // steps, m0 // 2 + i % steps, 0, at)),
        pl.BlockSpec((width, cols), lambda i: (0, 0)),
    ]
    kw = kept(h, args, in_specs, n)
    return call(
        functools.partial(final_kept_kernel, masks), 2 * rows * width * cols, 6 * rows * cols, 33,
        grid=(n,), in_specs=in_specs,
        out_specs=[pl.BlockSpec((1, cap, cols), functools.partial(lambda q, i: (jnp.where(i >= steps + q, 1, 0), 0, 0), m // 2)) for m in range(n)]
        + [pl.BlockSpec(memory_space=pltpu.VMEM)],
        out_shape=[jax.ShapeDtypeStruct((2, cap, cols), BF16)] * n + [pltpu.VMEM(h.shape, BF16)], **kw,
    )(*args)


def slot_of(info, e):
    return info[0, :, e:e + 1].astype(jnp.int32)


def gate_of(info, e):
    return info[0, :, INFO // 2 + e:INFO // 2 + e + 1]


def picked(k, groups, info, lo):
    slots = lax.broadcasted_iota(jnp.int32, (TB, WIN), 1)
    totals = [None] * len(groups)
    for m in range(MASKS):
        e = 2 * m + k
        at = pl.multiple_of(lo[m], 16)
        onehot = (slots == slot_of(info, e) - at).astype(BF16)
        for j, ys in enumerate(groups):
            term = gate_of(info, e) * mm(onehot, ys[m][0, pl.ds(at, WIN)])
            totals[j] = term if totals[j] is None else totals[j] + term
    return totals


def combine_kernel(k, n, held, first, last, *refs):
    total = refs[-1]
    refs = refs[:-2] if held else refs[:-1]
    groups = [refs[MASKS * j:MASKS * (j + 1)] for j in range(n)]
    info = refs[MASKS * n]
    cap, cols = groups[0][0].shape[1:]
    i, blocks = pl.program_id(0), pl.num_programs(0) // 2
    begin = [(jnp.minimum(first[i * MASKS + m], cap - WIN) // 16) * 16 for m in range(MASKS)]
    for j, part in enumerate(picked(k, groups, info, begin)):
        total[:, j * cols:(j + 1) * cols] = part
    slots = lax.broadcasted_iota(jnp.int32, (TB, WIN), 1)
    for m in range(MASKS):
        e = 2 * m + k
        end = last[i * MASKS + m]

        @pl.when(end > begin[m] + WIN)
        def _():
            def more(step, carry):
                lo = begin[m] + WIN + step * WIN
                at = pl.multiple_of(jnp.minimum(lo, cap - WIN), 16)
                mine = slot_of(info, e)
                onehot = (slots == jnp.where(mine >= lo, mine - at, -1)).astype(BF16)
                for j, ys in enumerate(groups):
                    total[:, j * cols:(j + 1) * cols] += gate_of(info, e) * mm(onehot, ys[m][0, pl.ds(at, WIN)])
                return carry

            lax.fori_loop(0, (end - begin[m] - 1) // WIN, more, 0)

    if k == 0:
        refs[-1][...] = total[...]
        return
    result = (refs[MASKS * n + 1][...] + total[...]).astype(BF16)
    for b, out in enumerate(refs[-2:]):

        @pl.when(i // blocks == b)
        def _():
            out[...] = result


def combine(groups, table, k, lo, model, acc=None, into=None, held=None):
    info, first, last = table
    _, cap, cols = groups[0][0].shape
    n, wide = len(groups), cols * len(groups)
    toks = info.shape[1]
    blocks = toks // TB
    at = lo // wide
    args = [first[k], last[k]] + [y for ys in groups for y in ys] + [info]
    in_specs = [pl.BlockSpec((1, cap, cols), lambda i, *_: (i // blocks, 0, 0))] * (MASKS * n)
    in_specs += [pl.BlockSpec((1, TB, INFO), lambda i, *_: (i // blocks, i % blocks, 0))]
    aliases = {}
    if k == 0:
        if into is not None:
            aliases |= filled_further(into, args, in_specs)["input_output_aliases"]
        out_specs = pl.BlockSpec((TB, wide), lambda i, *_: (i, at))
        out_shape = jax.ShapeDtypeStruct((2 * toks, model), F32)
    else:
        args.append(acc)
        in_specs.append(pl.BlockSpec((TB, wide), lambda i, *_: (i, at)))
        if into is not None:
            aliases = {len(args): 0, len(args) + 1: 1}
            args += into
            in_specs += [pl.BlockSpec(memory_space=pl.ANY)] * 2
        out_specs = [
            pl.BlockSpec((TB, wide), lambda i, *_: (jnp.minimum(i, blocks - 1), at)),
            pl.BlockSpec((TB, wide), lambda i, *_: (jnp.maximum(i - blocks, 0), at)),
        ]
        out_shape = [jax.ShapeDtypeStruct((toks, model), BF16)] * 2
        if held is not None:
            aliases |= kept(held, args, in_specs, 2)["input_output_aliases"]
            out_specs.append(pl.BlockSpec(memory_space=pltpu.VMEM))
            out_shape.append(pltpu.VMEM(held.shape, BF16))
    return call(
        functools.partial(combine_kernel, k, n, held is not None),
        2 * 2 * toks * MASKS * WIN * wide, 2 * toks * wide * 6, 33 if k else 20,
        grid_spec=pltpu.PrefetchScalarGridSpec(
            num_scalar_prefetch=2, grid=(2 * blocks,), in_specs=in_specs, out_specs=out_specs,
            scratch_shapes=[pltpu.VMEM((TB, wide), F32)],
        ),
        out_shape=out_shape, input_output_aliases=aliases,
    )(*args)


def cuts(sizes):
    out, at = [], 0
    for size in sizes:
        out.append((at, at + size))
        at += size
    return out


def solution(mesh):
    ep_size = mesh.shape["ep"]
    row_spec = P(("dp", "ep", "tp"), None)
    gate_spec = P("ep", None, "tp")
    down_spec = P("ep", "tp", None)
    up1_cuts = cuts([256, 1280, 768, 512])
    down_cuts = [cuts([1024, 512, 512]), cuts([256] * 7 + [128, 128])]
    late = [(1, n) for n in range(9)]
    halves = [(1, n) for n in range(5, 9)]
    after = {(1, 2): [[(1, 0), (1, 1)]], (1, 4): [[(1, 2)]], (1, 5): [[(1, 3)]], (1, 6): [[(1, 4), (1, 5)]]}
    after[1, 8] = [[(1, 6)], [(1, 7), (1, 8)]]

    def ep_swap(value, mask):
        return lax.ppermute(value, "ep", [(i, i ^ mask) for i in range(ep_size)])

    def tp_swap(w, k, lo=0, hi=None):
        piece = lax.slice(w, (k, 0, lo), (k + 1, w.shape[1], w.shape[2] if hi is None else hi))
        return lax.ppermute(piece, "tp", TP_SWAP)[0]

    def routing(ids, gates, me):
        toks, top_k = ids.shape[1:]
        n_exp = 2 * ep_size
        mean_load = top_k * toks // n_exp
        cap = mean_load + mean_load // 4
        code = ((ids // 2) ^ me) * 2 + ids % 2
        hit = code[:, None] == jnp.arange(n_exp, dtype=jnp.int32)[None, :, None, None]
        has = jnp.any(hit, axis=3)
        count = has.astype(jnp.int32)
        pos = jnp.cumsum(count, axis=2) - count
        pos = jnp.where(has & (pos < cap), pos, -1)
        gate = jnp.sum(jnp.where(hit, gates[:, None], 0.0), axis=3)
        used = jnp.sum(count.reshape(2, n_exp, toks // TB, TB), axis=3)
        upto = jnp.cumsum(used, axis=2)
        first, last = jnp.minimum(upto - used, cap), jnp.minimum(upto, cap)
        order = lambda a: a.reshape(2, ep_size, 2, toks // TB).transpose(2, 0, 3, 1).reshape(2, -1)
        return pos, gate, cap, order(first), order(last)

    def group_body(tokens_a, ids_a, gates_a, tokens_b, ids_b, gates_b, w_gate, w_up, w_down):
        me = lax.axis_index("ep")
        model = w_down.shape[2]
        up1 = [None] * len(up1_cuts)
        up1[0] = tp_swap(w_up, 1, *up1_cuts[0])
        gate0 = tp_swap(w_gate, 0)
        up0 = tp_swap(w_up, 0)
        down = [[None] * len(c) for c in down_cuts]
        for n, (lo, hi) in enumerate(down_cuts[0]):
            down[0][n] = tp_swap(w_down, 0, lo, hi)
        gate1 = tp_swap(w_gate, 1)
        for n, (lo, hi) in list(enumerate(up1_cuts))[1:]:
            up1[n] = tp_swap(w_up, 1, lo, hi)
        for k, n in late:
            lo, hi = down_cuts[k][n]
            down[k][n] = tp_swap(w_down, k, lo, hi)

        pos, gate, cap, first, last = routing(jnp.stack([ids_a, ids_b]), jnp.stack([gates_a, gates_b]), me)
        info = [jnp.pad(a, ((0, 0), (0, INFO // 2 - a.shape[1]), (0, 0))) for a in (pos.astype(F32), gate)]
        table = jnp.concatenate(info, axis=1).transpose(0, 2, 1), first, last

        xs = []
        for b, tokens in enumerate((tokens_a, tokens_b)):
            rows = pos[b][:, None, :]
            far = dispatch(rows[4:], tokens, cap)
            far = [ep_swap(far[0], 2), ep_swap(far[1], 3)]
            near = dispatch(rows[:4], tokens, cap)
            xs.append([near[0], ep_swap(near[1], 1), *far])
        p, h_l = None, []
        for b in range(2):
            h_l.append(hidden_local(xs[b], w_gate, w_up))
        for b in range(2):
            p = part(h_l[b], b, w_down, p)

        h_r = [None, None]
        for b in range(2):
            h_r[0] = hidden(xs[b], b, 0, gate0, up0, 0, h_r[0])
        for n, (lo, hi) in enumerate(up1_cuts):
            for b in range(2):
                h_r[1] = hidden(xs[b], b, 1, gate1, up1[n], lo, h_r[1])

        acc, outs, back = None, None, {}

        def finish(k, n):
            lo, _ = down_cuts[k][n]
            if (k, n) in halves:
                *far, h_r[k] = final_kept(h_r[k], p, k, down[k][n], lo, (2, 3))
                *near, h_r[k] = final_kept(h_r[k], p, k, down[k][n], lo, (0, 1))
            else:
                if k == 0:
                    ys = final(h_r[k], p, k, down[k][n], lo)
                else:
                    *ys, h_r[k] = final_kept(h_r[k], p, k, down[k][n], lo, (0, 1, 2, 3))
                near, far = ys[:2], ys[2:]
            far = [ep_swap(far[0], 2), ep_swap(far[1], 3)]
            near = [near[0], ep_swap(near[1], 1)]
            back[k, n] = near + far

        for item in (0, 0), (0, 1), (0, 2):
            finish(*item)
            acc = combine([back[item]], table, 0, down_cuts[0][item[1]][0], model, None, acc)
        for i, item in enumerate(late):
            finish(*item)
            for group in after.get(item, []):
                outs = combine(
                    [back[it] for it in group], table, 1, down_cuts[1][group[0][1]][0], model, acc, outs,
                    h_r[1] if i < len(late) - 1 else None,
                )
                if i < len(late) - 1:
                    *outs, h_r[1] = outs
        return tuple(outs)

    in_specs = (row_spec, row_spec, row_spec, row_spec, row_spec, row_spec, gate_spec, gate_spec, down_spec)
    return jax.shard_map(group_body, mesh=mesh, in_specs=in_specs, out_specs=(row_spec, row_spec), check_vma=False)
```
